32 devices in a mesh: gx: 4 (over y, x), gy: 4 (over z), gz: 2 (over core).
Axes of the slice: x: 2, y: 2, z: 4, core: 2. Of those that a mesh axis runs over, the one named last changes fastest.
Arguments:
- rhs: bfloat16 [2, 4096, 4096], P('gz', 'gx', 'gy'), may hold values from -40 to 40
- basis_x: bfloat16 [4096, 4096], P('gx', ('gy', 'gz')), may hold values from -0.125 to 0.125
- basis_y: bfloat16 [4096, 4096], P('gy', ('gx', 'gz')), may hold values from -0.125 to 0.125
- eig_x: float32 [4096], P('gx'), may hold values from 0.1 to 4
- eig_y: float32 [4096], P('gy'), may hold values from 0.1 to 4
- eig_z: float32 [2], P('gz'), may hold values from 0.1 to 4
Outputs:
- solution: bfloat16 [2, 4096, 4096], P('gz', 'gx', 'gy')
- energy: float32 [], replicated
The draws below stay inside these ranges and needn't reach their ends.
All inputs are finite; a program needn't handle non-finite values.
Results may differ from the reference program's by a relative error of at most 0.01.
Values may be sent and summed in bfloat16 or wider, within the bound.
A program may use at most 128 MiB of HBM per device.

```python
import math
import jax
import jax.numpy as jnp

NX = 4096
NY = 4096
KZ = 2


def draw_rhs(key, part):
    first_key, second_key = jax.random.split(jax.random.fold_in(key, 17))
    position = jnp.arange(NX, dtype=jnp.float32) / NX
    rough = jnp.exp(jax.random.uniform(second_key, (NX,), jnp.float32, -0.7, 0.7))
    values = jnp.clip(jax.random.normal(first_key, (KZ, NX, NY), jnp.float32), -6.0, 6.0)
    trend = jnp.exp(jnp.log(3.0) * position)
    return (values * (trend * rough)[None, :, None]).astype(jnp.bfloat16)


def with_spikes(drawn, key, source, target, shards_of, factor):
    owner, partner = [(jnp.arange(drawn.shape[dim]) // (drawn.shape[dim] // shards_of)).reshape([-1 if axis == dim else 1 for axis in range(drawn.ndim)]) for dim in (source, target)]
    chosen = jax.random.permutation(key, shards_of)[partner]
    strong = (owner == chosen) | (owner == (partner + shards_of // 2) % shards_of)
    return jnp.where(strong, factor * drawn, drawn)


def levels(own_key, extent, shards, smallest, largest):
    gain = 1.0
    for dim, shards_of in shards:
        heights = jax.random.uniform(jax.random.fold_in(jax.random.fold_in(own_key, 6), dim), (shards_of,), jnp.float32, smallest / len(shards), largest / len(shards))
        gain = gain * jnp.repeat(jnp.exp(heights), extent[dim] // shards_of).reshape((-1,) + (1,) * (len(extent) - 1 - dim))
    return gain


def gaussian_with(key, extent, spread, bound, cuts, heavy, held_as=jnp.bfloat16):
    array = spread * jax.random.normal(key, extent, jnp.float32)
    if cuts:
        array = array * levels(key, extent, cuts, -0.22, 0.18)
    return jnp.clip(with_spikes(array, jax.random.fold_in(key, 3), *heavy), -bound, bound).astype(held_as)


def setup_inputs(seed: int = 0) -> dict:
    arg_keys = jax.random.split(jax.random.key(seed), 7)
    return {
        "rhs": draw_rhs(jax.random.fold_in(arg_keys[6], 71), 0),
        "basis_x": gaussian_with(arg_keys[1], (NX, NX), NX ** -0.5, 0.125, ((0, 4), (1, 8)), (0, 1, 8, 2.0)),
        "basis_y": gaussian_with(arg_keys[2], (NY, NY), NY ** -0.5, 0.125, ((0, 4), (1, 8)), (0, 1, 8, 2.0)),
        "eig_x": jnp.clip(jnp.exp(math.log(4.0) - 3.6888794 * jax.random.uniform(arg_keys[3], (NX,), jnp.float32) ** levels(arg_keys[3], (NX,), ((0, 4),), -0.2, 0.2)), 0.1, 4.0),
        "eig_y": jnp.clip(jnp.exp(math.log(4.0) - 3.6888794 * jax.random.uniform(arg_keys[4], (NY,), jnp.float32) ** levels(arg_keys[4], (NY,), ((0, 4),), -0.2, 0.2)), 0.1, 4.0),
        "eig_z": jnp.clip(jnp.exp(math.log(4.0) - 3.6888794 * jax.random.uniform(arg_keys[5], (KZ,), jnp.float32) ** levels(arg_keys[5], (KZ,), ((0, 2),), -0.2, 0.2)), 0.1, 4.0),
    }


def reference(rhs, basis_x, basis_y, eig_x, eig_y, eig_z):
    basis_xf = basis_x.astype(jnp.float32)
    basis_yf = basis_y.astype(jnp.float32)
    rhs_wide = rhs.astype(jnp.float32)
    section_g = jnp.einsum('xi,kxy->kiy', basis_xf, rhs_wide).astype(jnp.bfloat16)
    section_h = jnp.einsum('yj,kiy->kij', basis_yf, section_g.astype(jnp.float32))
    denominator = eig_z[:, None, None] + eig_x[None, :, None] + eig_y[None, None, :]
    scaled = (section_h / denominator).astype(jnp.bfloat16)
    section_v = jnp.einsum('yj,kij->kiy', basis_yf, scaled.astype(jnp.float32)).astype(jnp.bfloat16)
    section_s = jnp.einsum('xi,kiy->kxy', basis_xf, section_v.astype(jnp.float32))
    return section_s.astype(jnp.bfloat16), jnp.sum(rhs_wide * section_s)
```

```python
import functools

import jax
import jax.numpy as jnp
from jax import lax
from jax.experimental import pallas as pl
from jax.experimental.pallas import tpu as pltpu
from jax.sharding import PartitionSpec as P

BF16, F32 = jnp.bfloat16, jnp.float32
LANES = 128


def contract(left, right, dims):
    return lax.dot_general(left, right, ((dims[:1], dims[1:]), ((), ())), preferred_element_type=F32)


def kernel(
    nx, ny, yq,
    rhs, bx, by, ex, ey, ez,
    out, energy,
    bxb, byb, wide, gs, grecv, gall, wbuf, vrecv, vfull, sown, srecv,
    exall, eyall, ezall, dcol, eacc, e1, e2, e3,
    s_loc, s_eig, r_eig, s_head, r_head, s_bxz, r_bxz, s_bxd, r_bxd, s_byz, r_byz, s_byp, r_byp,
    s_g, r_g, s_ga, r_ga, s_gd, r_gd, s_vd, r_vd, s_va, r_va, s_vb, r_vb, s_s, r_s, s_out, s_e, r_e,
):
    p, z, c = lax.axis_index("gx"), lax.axis_index("gy"), lax.axis_index("gz")
    px, py = p % 2, p // 2
    nb = nx // 2
    xb, yb = rhs.shape[1], rhs.shape[2]
    cx, cy = bx.shape[1], by.shape[1]
    ci = cx // 2
    ib = ci // nb
    chunks = yb // yq
    half = yb // 2
    other = 1 - c

    def remote(src, dst, ss, rs, **where):
        return pltpu.make_async_remote_copy(
            src_ref=src, dst_ref=dst, send_sem=ss, recv_sem=rs,
            device_id=where, device_id_type=pl.DeviceIdType.MESH,
        )

    def loop(count, body):
        lax.fori_loop(0, count, lambda i, carry: (body(i), carry)[1], 0)

    def cols(start, size):
        return pl.ds(pl.multiple_of(start, LANES), size)

    def rows(start, size):
        return pl.ds(pl.multiple_of(start, size), size)

    barrier = pltpu.get_barrier_semaphore()
    for t in range(1, nx):
        pl.semaphore_signal(barrier, inc=1, device_id={"gx": p ^ t}, device_id_type=pl.DeviceIdType.MESH)
    for d in range(1, ny):
        pl.semaphore_signal(barrier, inc=1, device_id={"gy": (z + d) % ny}, device_id_type=pl.DeviceIdType.MESH)
    pl.semaphore_signal(barrier, inc=1, device_id={"gz": other}, device_id_type=pl.DeviceIdType.MESH)

    mine = rows(px * xb, xb)
    theirs = rows((1 - px) * xb, xb)
    local = [
        pltpu.make_async_copy(by, byb.at[z, p], s_loc.at[0]),
        pltpu.make_async_copy(rhs.at[0], wide.at[mine, :], s_loc.at[1]),
        pltpu.make_async_copy(bx.at[:, cols(px * ci, ci)], bxb.at[z, c, mine, :], s_loc.at[2]),
        pltpu.make_async_copy(ex, exall.at[p], s_loc.at[3]),
        pltpu.make_async_copy(ey, eyall.at[z], s_loc.at[4]),
        pltpu.make_async_copy(ez, ezall.at[c], s_loc.at[5]),
    ]
    for copy in local:
        copy.start()
    pl.semaphore_wait(barrier, nx + ny - 1)

    swap_bx = remote(bx.at[:, cols((1 - px) * ci, ci)], bxb.at[z, c, mine, :], s_head.at[0], r_head.at[0], gx=p ^ 1)
    swap_bx.start()
    for copy in local:
        copy.wait()
    eigs = [remote(exall.at[p], exall.at[p], s_eig.at[t], r_eig.at[t], gx=p ^ t) for t in range(1, nx)]
    eigs += [
        remote(eyall.at[z], eyall.at[z], s_eig.at[nx + d], r_eig.at[nx + d], gy=(z + d) % ny) for d in range(1, ny)
    ]
    eigs += [remote(ezall.at[c], ezall.at[c], s_eig.at[0], r_eig.at[0], gz=other)]
    for copy in eigs:
        copy.start()
    swap_rhs = remote(wide.at[mine, :], wide.at[mine, :], s_head.at[1], r_head.at[1], gx=p ^ 1)

    def line(buffer, ss, rs, zs, up, index):
        ref = buffer.at[(zs,) + index]
        return remote(ref, ref, ss.at[zs, 0 if up else 1], rs.at[zs], gy=jnp.clip(z + (1 if up else -1), 0, ny - 1))

    def bx_line(zs, up):
        return line(bxb, s_bxz, r_bxz, zs, up, (c,))

    def by_line(zs, up):
        return line(byb, s_byz, r_byz, zs, up, (p,))

    def goes_on(up):
        return z + 1 < ny if up else z > 0

    def source(r, up):
        zs = z - r if up else z + r
        return zs, jnp.logical_and(zs >= 0, zs < ny)

    def bx_pass(zs):
        return remote(bxb.at[zs, c], bxb.at[zs, c], s_bxd.at[zs], r_bxd.at[zs], gz=other)

    def piece(zs, owner, part):
        return byb.at[zs, owner, pl.ds(part * half, half), :]

    def plane_copies(zs):
        direct, relay = [], []
        slot = 0
        for b in range(nb):
            t = 2 * b if b else 1
            for part in (0, 1) if t == 1 else (1, 0):
                ref = piece(zs, p, part)
                direct.append(remote(ref, ref, s_byp.at[zs, slot], r_byp.at[zs, t, part], gx=p ^ t))
                slot += 1
        for b in range(1, nb):
            ref = piece(zs, p ^ 1, 0)
            relay.append(((1, 0), remote(ref, ref, s_byp.at[zs, slot], r_byp.at[zs, 2 * b + 1, 0], gx=p ^ (2 * b))))
            slot += 1
        for b in range(1, nb):
            ref = piece(zs, p ^ (2 * b), 1)
            relay.append(((2 * b, 1), remote(ref, ref, s_byp.at[zs, slot], r_byp.at[zs, 2 * b + 1, 1], gx=p ^ 1)))
            slot += 1
        return direct, relay

    def wait_piece(zs, t, part):
        ref = piece(zs, p ^ t, part)
        remote(ref, ref, s_byp.at[zs, 0], r_byp.at[zs, t, part], gx=p ^ 1).wait_recv()

    def relays(zs):
        seen = set()
        for key, copy in plane_copies(zs)[1]:
            if key not in seen:
                seen.add(key)
                wait_piece(zs, *key)
            copy.start()

    def g_copies(zs):
        return [
            remote(gs.at[zs, py ^ b], grecv.at[zs, b - 1], s_g.at[zs, b - 1], r_g.at[zs, b - 1], gx=p ^ (2 * b))
            for b in range(1, nb)
        ]

    def first(zs):
        bx_pass_in(zs).wait_recv()

        def tile(i):
            cc, n = i // (yb // yq), i % (yb // yq)
            part = contract(bxb[zs, cc], wide[:, cols(n * yq, yq)], (0, 0)).astype(BF16)
            for b in range(nb):
                gs[zs, b, cc, :, cols(n * yq, yq)] = part[b * ib : (b + 1) * ib]

        loop(2 * (yb // yq), tile)
        for copy in g_copies(zs):
            copy.start()

    def bx_pass_in(zs):
        return remote(bxb.at[zs, other], bxb.at[zs, other], s_bxd.at[zs], r_bxd.at[zs], gz=other)

    def g_send(zs):
        return remote(gs.at[zs, py], gall.at[z, c], s_ga.at[zs], r_ga.at[z], gy=zs)

    def g_pass(zs, core):
        return remote(gall.at[zs, core], gall.at[zs, core], s_gd.at[zs], r_gd.at[zs], gz=other)

    def collect(zs):
        for copy in g_copies(zs):
            copy.wait_recv()

        def tile(i):
            cc, n = i // (yb // yq), i % (yb // yq)
            lanes = cols(n * yq, yq)
            total = gs[zs, py, cc, :, lanes].astype(F32)
            for b in range(1, nb):
                total = total + grecv[zs, b - 1, cc, :, lanes].astype(F32)

            @pl.when(zs != z)
            def _():
                gs[zs, py, cc, :, lanes] = total.astype(BF16)

            @pl.when(zs == z)
            def _():
                gall[z, c, cc, :, lanes] = total.astype(BF16)

        loop(2 * (yb // yq), tile)

        @pl.when(zs != z)
        def _():
            g_send(zs).start()

        @pl.when(zs == z)
        def _():
            g_pass(z, c).start()

    def start_line(maker, zs, r):
        for up in (True, False):
            @pl.when(goes_on(up))
            def _(up=up):
                maker(zs, up).start()

    def start_plane(zs):
        for copy in plane_copies(zs)[0]:
            copy.start()

    start_line(by_line, z, 0)
    swap_rhs.start()
    start_plane(z)
    remote(bx.at[:, cols(px * ci, ci)], bxb.at[z, c, theirs, :], s_head.at[0], r_head.at[0], gx=p ^ 1).wait_recv()
    start_line(bx_line, z, 0)
    bx_pass(z).start()

    def forward(maker, r, then):
        for up in (True, False):
            zs, valid = source(r, up)

            @pl.when(valid)
            def _(zs=zs, up=up):
                maker(zs, up).wait_recv()

                @pl.when(goes_on(up))
                def _():
                    maker(zs, up).start()

                then(zs)

    def each(r, act):
        for up in (True, False):
            zs, valid = source(r, up)
            valid = jnp.logical_and(valid, r >= 0)
            if not up:
                valid = jnp.logical_and(valid, r > 0)

            @pl.when(valid)
            def _(zs=zs):
                act(zs)

    def round_of(i):
        r = i + 1
        forward(bx_line, r, lambda zs: bx_pass(zs).start())

        @pl.when(r == 1)
        def _():
            remote(wide.at[theirs, :], wide.at[theirs, :], s_head.at[1], r_head.at[1], gx=p ^ 1).wait_recv()

        each(r - 1, first)
        each(r - 2, relays)
        each(r - 2, collect)
        forward(by_line, r, start_plane)

    loop(ny + 1, round_of)

    for t in range(1, nx):
        remote(exall.at[p ^ t], exall.at[p ^ t], s_eig.at[t], r_eig.at[t], gx=p ^ t).wait_recv()
    for d in range(1, ny):
        far = (z - d) % ny
        remote(eyall.at[far], eyall.at[far], s_eig.at[nx + d], r_eig.at[nx + d], gy=(z + d) % ny).wait_recv()
    remote(ezall.at[other], ezall.at[other], s_eig.at[0], r_eig.at[0], gz=other).wait_recv()
    for cc in range(2):
        start = (z * 2 + cc) * cx + px * ci + py * ib
        line_at = start // LANES
        per = xb // LANES
        row = exall[line_at // per, pl.ds(line_at % per, 1), :]
        lane = lax.broadcasted_iota(jnp.int32, (ib, LANES), 1)
        want = lax.broadcasted_iota(jnp.int32, (ib, LANES), 0) + start % LANES
        column = jnp.sum(jnp.where(lane == want, jnp.broadcast_to(row, (ib, LANES)), 0.0), axis=1, keepdims=True)
        for k in range(2):
            dcol[pl.ds((k * 2 + cc) * ib, ib), :] = jnp.broadcast_to(column, (ib, LANES)) + ezall[k, 0:1, :]

    def arrive(d):
        zs = (z + 1 + d) % ny
        remote(gall.at[zs, c], gall.at[zs, c], s_ga.at[zs], r_ga.at[zs], gy=zs).wait_recv()
        g_pass(zs, c).start()

    loop(ny - 1, arrive)

    def passed(zs):
        g_pass(zs, other).wait_recv()

    loop(ny, passed)
    eacc[...] = jnp.zeros_like(eacc)

    tn = min(cy, 256)

    def second(t):
        owner = p ^ t

        def landed(zs):
            @pl.when(t % 2 == 1)
            def _():
                wait_piece(zs, t, 1)

            @pl.when(t > 1)
            def _():
                wait_piece(zs, t, 0)

        loop(ny, landed)

        def tile(n):
            h = None
            for zs in range(ny):
                term = contract(gall[zs].reshape(4 * ib, yb), byb[zs, owner, :, cols(n * tn, tn)], (1, 0))
                h = term if h is None else h + term
            for l in range(tn // LANES):
                line_at = ((owner * 2 + c) * cy + n * tn) // LANES + l
                per = yb // LANES
                row = eyall[line_at // per, pl.ds(line_at % per, 1), :]
                part = h[:, l * LANES : (l + 1) * LANES]
                w = part / (dcol[...] + row)
                eacc[...] += jnp.sum((part * w).reshape(-1, 8, LANES), axis=0)
                wbuf[owner, :, cols(n * tn + l * LANES, LANES)] = w.astype(BF16)

        loop(cy // tn, tile)

    loop(nx, second)

    def v_pass(q, zs, core):
        lanes = cols(q * yq, yq)
        return remote(gall.at[zs, core, :, :, lanes], vrecv.at[zs, :, :, lanes], s_vd.at[q, zs], r_vd.at[q, zs], gz=other)

    def v_slot(q, zs, owner):
        return vfull.at[q, zs, :, pl.ds(pl.multiple_of(owner * ib, ib), ib), :]

    def v_send(q, zs):
        return remote(
            gall.at[zs, c, :, :, cols(q * yq, yq)], v_slot(q, z, py), s_va.at[q, zs], r_va.at[q, z], gy=zs
        )

    def v_copies(q, zs):
        return [
            remote(v_slot(q, zs, py), v_slot(q, zs, py), s_vb.at[q, zs, b - 1], r_vb.at[q, zs, b - 1], gx=p ^ (2 * b))
            for b in range(1, nb)
        ]

    def third(q):
        def target(d):
            zs = (z + 1 + d) % ny
            v = None
            for owner in range(nx):
                term = contract(wbuf[owner], byb[zs, owner, rows(q * yq, yq), :], (1, 1))
                v = term if v is None else v + term
            gall[zs, :, :, :, cols(q * yq, yq)] = v.astype(BF16).reshape(2, 2, ib, yq)
            v_pass(q, zs, other).start()

        loop(ny, target)

    def merge(q):
        def target(d):
            zs = (z + 1 + d) % ny
            lanes = cols(q * yq, yq)
            v_pass(q, zs, c).wait_recv()
            v = (gall[zs, c, :, :, lanes].astype(F32) + vrecv[zs, :, :, lanes].astype(F32)).astype(BF16)

            @pl.when(zs != z)
            def _():
                gall[zs, c, :, :, lanes] = v
                v_send(q, zs).start()

            @pl.when(zs == z)
            def _():
                vfull[q, zs, :, pl.ds(pl.multiple_of(py * ib, ib), ib), :] = v

        loop(ny, target)

    def spread(q):
        def target(d):
            zs = (z + d) % ny

            @pl.when(zs != z)
            def _():
                remote(v_slot(q, zs, py), v_slot(q, zs, py), s_va.at[q, zs], r_va.at[q, zs], gy=zs).wait_recv()

            for copy in v_copies(q, zs):
                copy.start()

        loop(ny, target)

    mt = min(xb, 512)

    def s_copy(q):
        lanes = cols(q * yq, yq)
        return remote(wide.at[theirs, lanes], srecv.at[:, lanes], s_s.at[q], r_s.at[q], gx=p ^ 1)

    def fourth(q):
        lanes = cols(q * yq, yq)

        def landed(zs):
            for b in range(1, nb):
                slot = v_slot(q, zs, py ^ b)
                remote(slot, slot, s_vb.at[q, zs, b - 1], r_vb.at[q, zs, b - 1], gx=p ^ (2 * b)).wait_recv()

        loop(ny, landed)

        def tile(i):
            m, own = i % (xb // mt), i // (xb // mt)
            side = jnp.where(own == 1, px, 1 - px)
            at = rows(side * xb + m * mt, mt)
            s = None
            for zs in range(ny):
                for cc in range(2):
                    term = contract(bxb[zs, cc, at, :], vfull[q, zs, cc], (1, 0))
                    s = term if s is None else s + term

            @pl.when(own == 0)
            def _():
                wide[at, lanes] = s.astype(BF16)

                @pl.when(m == xb // mt - 1)
                def _():
                    s_copy(q).start()

            @pl.when(own == 1)
            def _():
                sown[rows(m * mt, mt), lanes] = s

        loop(2 * (xb // mt), tile)

    def out_copy(q):
        lanes = cols(q * yq, yq)
        return pltpu.make_async_copy(wide.at[mine, lanes], out.at[0, :, lanes], s_out.at[q])

    def finish(q):
        lanes = cols(q * yq, yq)
        s_copy(q).wait_recv()

        def tile(m):
            at = rows(m * mt, mt)
            wide[rows(px * xb + m * mt, mt), lanes] = (sown[at, lanes] + srecv[at, lanes].astype(F32)).astype(BF16)

        loop(xb // mt, tile)
        out_copy(q).start()

    def left(zs):
        g_pass(zs, c).wait_send()

    loop(ny, left)
    swap_rhs.wait_send()

    e_core = remote(eacc, e1, s_e.at[0], r_e.at[0], gz=other)
    e_plane = [remote(e2.at[p], e2.at[p], s_e.at[t], r_e.at[t], gx=p ^ t) for t in range(1, nx)]
    e_line = [remote(e3.at[z], e3.at[z], s_e.at[nx + d], r_e.at[nx + d], gy=(z + d) % ny) for d in range(1, ny)]

    def leave(t):
        @pl.when(t == 0)
        def _():
            e_core.start()

        @pl.when(t == 1)
        def _():
            e_core.wait_recv()
            e2[p] = eacc[...] + e1[...]
            for copy in e_plane:
                copy.start()

        @pl.when(t == 2)
        def _():
            for s in range(1, nx):
                remote(e2.at[p ^ s], e2.at[p ^ s], s_e.at[s], r_e.at[s], gx=p ^ s).wait_recv()
            total = e2[0]
            for s in range(1, nx):
                total = total + e2[s]
            e3[z] = total
            for copy in e_line:
                copy.start()

        @pl.when(t < chunks)
        def _():
            third(t)

        @pl.when(jnp.logical_and(t >= 1, t <= chunks))
        def _():
            merge(t - 1)

    loop(max(chunks + 1, 3), leave)

    def come(t):
        @pl.when(t < chunks)
        def _():
            spread(t)

        @pl.when(jnp.logical_and(t >= 1, t <= chunks))
        def _():
            fourth(t - 1)

        @pl.when(t >= 2)
        def _():
            finish(t - 2)

    loop(chunks + 2, come)

    for d in range(1, ny):
        far = (z - d) % ny
        remote(e3.at[far], e3.at[far], s_e.at[nx + d], r_e.at[nx + d], gy=(z + d) % ny).wait_recv()
    total = e3[0]
    for s in range(1, ny):
        total = total + e3[s]
    energy[...] = jnp.broadcast_to(jnp.sum(jnp.sum(total, axis=0, keepdims=True), axis=1, keepdims=True), energy.shape)

    swap_bx.wait_send()
    for copy in eigs + [e_core] + e_plane + e_line:
        copy.wait_send()

    def drain(zs):
        for up in (True, False):
            from_here = zs <= z if up else zs >= z

            @pl.when(jnp.logical_and(goes_on(up), from_here))
            def _(up=up):
                bx_line(zs, up).wait_send()
                by_line(zs, up).wait_send()

        bx_pass(zs).wait_send()
        direct, relay = plane_copies(zs)
        for copy in direct + [copy for _, copy in relay] + g_copies(zs):
            copy.wait_send()

        @pl.when(zs != z)
        def _():
            g_send(zs).wait_send()

        def chunk(q):
            v_pass(q, zs, other).wait_send()
            for copy in v_copies(q, zs):
                copy.wait_send()

            @pl.when(zs != z)
            def _():
                v_send(q, zs).wait_send()

        loop(chunks, chunk)

    loop(ny, drain)

    def drain_chunk(q):
        s_copy(q).wait_send()
        out_copy(q).wait()

    loop(chunks, drain_chunk)


def shards(nx, ny, rhs, basis_x, basis_y, eig_x, eig_y, eig_z):
    xb, yb = rhs.shape[1], rhs.shape[2]
    cx, cy = basis_x.shape[1], basis_y.shape[1]
    nb, ci = nx // 2, cx // 2
    ib = ci // nb
    yq = min(yb, 256)
    chunks = yb // yq
    ex = eig_x.reshape(xb // LANES, LANES)
    ey = eig_y.reshape(yb // LANES, LANES)
    ez = jnp.broadcast_to(eig_z.reshape(1, 1), (8, LANES))
    dma = pltpu.SemaphoreType.DMA
    any_space, vmem = pl.BlockSpec(memory_space=pl.ANY), pl.BlockSpec(memory_space=pltpu.VMEM)
    solution, energy = pl.pallas_call(
        functools.partial(kernel, nx, ny, yq),
        name="solve",
        out_shape=(
            jax.ShapeDtypeStruct(rhs.shape, BF16),
            jax.ShapeDtypeStruct((8, LANES), F32),
        ),
        in_specs=[any_space] * 3 + [vmem] * 3,
        out_specs=(any_space, vmem),
        scratch_shapes=[
            pltpu.VMEM((ny, 2, 2 * xb, ci), BF16),
            pltpu.VMEM((ny, nx, yb, cy), BF16),
            pltpu.VMEM((2 * xb, yb), BF16),
            pltpu.VMEM((ny, nb, 2, ib, yb), BF16),
            pltpu.VMEM((ny, nb - 1, 2, ib, yb), BF16),
            pltpu.VMEM((ny, 2, 2, ib, yb), BF16),
            pltpu.VMEM((nx, 4 * ib, cy), BF16),
            pltpu.VMEM((ny, 2, ib, yb), BF16),
            pltpu.VMEM((chunks, ny, 2, nb * ib, yq), BF16),
            pltpu.VMEM((xb, yb), F32),
            pltpu.VMEM((xb, yb), BF16),
            pltpu.VMEM((nx, xb // LANES, LANES), F32),
            pltpu.VMEM((ny, yb // LANES, LANES), F32),
            pltpu.VMEM((2, 8, LANES), F32),
            pltpu.VMEM((4 * ib, LANES), F32),
            pltpu.VMEM((8, LANES), F32),
            pltpu.VMEM((8, LANES), F32),
            pltpu.VMEM((nx, 8, LANES), F32),
            pltpu.VMEM((ny, 8, LANES), F32),
            dma((6,)),
            dma((nx + ny,)), dma((nx + ny,)),
            dma((2,)), dma((2,)),
            dma((ny, 2)), dma((ny,)),
            dma((ny,)), dma((ny,)),
            dma((ny, 2)), dma((ny,)),
            dma((ny, 4 * nb - 2)), dma((ny, nx, 2)),
            dma((ny, nb - 1)), dma((ny, nb - 1)),
            dma((ny,)), dma((ny,)),
            dma((ny,)), dma((ny,)),
            dma((chunks, ny)), dma((chunks, ny)),
            dma((chunks, ny)), dma((chunks, ny)),
            dma((chunks, ny, nb - 1)), dma((chunks, ny, nb - 1)),
            dma((chunks,)), dma((chunks,)),
            dma((chunks,)),
            dma((nx + ny,)), dma((nx + ny,)),
        ],
        compiler_params=pltpu.CompilerParams(
            collective_id=0, has_side_effects=True, vmem_limit_bytes=65472 * 1024
        ),
    )(rhs, basis_x, basis_y, ex, ey, ez)
    return solution, energy[0, 0]


def solution(mesh):
    return jax.shard_map(
        functools.partial(shards, mesh.shape["gx"], mesh.shape["gy"]),
        mesh=mesh,
        in_specs=(
            P("gz", "gx", "gy"),
            P("gx", ("gy", "gz")),
            P("gy", ("gx", "gz")),
            P("gx"),
            P("gy"),
            P("gz"),
        ),
        out_specs=(P("gz", "gx", "gy"), P()),
        check_vma=False,
    )
```

```python
import functools

import jax
import jax.numpy as jnp
from jax import lax
from jax.experimental import pallas as pl
from jax.experimental.pallas import tpu as pltpu
from jax.sharding import PartitionSpec as P

BF16, F32 = jnp.bfloat16, jnp.float32
LANES = 128


def contract(left, right, dims):
    return lax.dot_general(left, right, ((dims[:1], dims[1:]), ((), ())), preferred_element_type=F32)


def kernel(
    nx, ny, yq,
    rhs, bx, by, ex, ey, ez,
    out, energy,
    bxb, byb, wide, gs, grecv, gall, wbuf, vrecv, vfull, sown, srecv,
    exall, eyall, ezall, dcol, eacc, e1, e2, e3,
    s_loc, s_eig, r_eig, s_head, r_head, s_bxz, r_bxz, s_bxd, r_bxd, s_byf, r_byf, s_byc, r_byc, s_byp, r_byp,
    s_g, r_g, s_ga, r_ga, s_gd, r_gd, s_vd, r_vd, s_va, r_va, s_vb, r_vb, s_s, r_s, s_out, s_e, r_e,
):
    p, z, c = lax.axis_index("gx"), lax.axis_index("gy"), lax.axis_index("gz")
    px, py = p % 2, p // 2
    nb = nx // 2
    xb, yb = rhs.shape[1], rhs.shape[2]
    cx, cy = bx.shape[1], by.shape[1]
    ci = cx // 2
    ib = ci // nb
    chunks = yb // yq
    half = yb // 2
    other = 1 - c
    mid = ny // 2
    low = z < mid
    works = jnp.logical_or(z == mid - 1, z == mid)
    rests = jnp.logical_not(works)
    place = jnp.where(low, 0, 1)

    def when(condition, act):
        @pl.when(condition)
        def _():
            act()

    def remote(src, dst, ss, rs, **where):
        return pltpu.make_async_remote_copy(
            src_ref=src, dst_ref=dst, send_sem=ss, recv_sem=rs,
            device_id=where, device_id_type=pl.DeviceIdType.MESH,
        )

    def loop(count, body):
        lax.fori_loop(0, count, lambda i, carry: (body(i), carry)[1], 0)

    def cols(start, size):
        return pl.ds(pl.multiple_of(start, LANES), size)

    def rows(start, size):
        return pl.ds(pl.multiple_of(start, size), size)

    barrier = pltpu.get_barrier_semaphore()
    for t in range(1, nx):
        pl.semaphore_signal(barrier, inc=1, device_id={"gx": p ^ t}, device_id_type=pl.DeviceIdType.MESH)
    for d in range(1, ny):
        pl.semaphore_signal(barrier, inc=1, device_id={"gy": (z + d) % ny}, device_id_type=pl.DeviceIdType.MESH)
    pl.semaphore_signal(barrier, inc=1, device_id={"gz": other}, device_id_type=pl.DeviceIdType.MESH)

    mine = rows(px * xb, xb)
    theirs = rows((1 - px) * xb, xb)
    local = [
        pltpu.make_async_copy(by, byb.at[z, p], s_loc.at[0]),
        pltpu.make_async_copy(rhs.at[0], wide.at[mine, :], s_loc.at[1]),
        pltpu.make_async_copy(bx.at[:, cols(px * ci, ci)], bxb.at[z, c, mine, :], s_loc.at[2]),
        pltpu.make_async_copy(ex, exall.at[p], s_loc.at[3]),
        pltpu.make_async_copy(ey, eyall.at[z], s_loc.at[4]),
    ]
    for copy in local:
        copy.start()
    pl.semaphore_wait(barrier, nx + ny - 1)

    swap_bx = remote(bx.at[:, cols((1 - px) * ci, ci)], bxb.at[z, c, mine, :], s_head.at[0], r_head.at[0], gx=p ^ 1)
    swap_bx.start()
    swap_rhs = remote(wide.at[mine, :], wide.at[mine, :], s_head.at[1], r_head.at[1], gx=p ^ 1)
    eigs = [remote(exall.at[p], exall.at[p], s_eig.at[t], r_eig.at[t], gx=p ^ t) for t in range(1, nx)]
    eigs += [
        remote(eyall.at[z], eyall.at[z], s_eig.at[nx + d], r_eig.at[nx + d], gy=(z + d) % ny) for d in range(1, ny)
    ]
    eigs += [remote(ezall.at[c], ezall.at[c], s_eig.at[0], r_eig.at[0], gz=other)]

    def line(buffer, ss, rs, zs, up, index):
        ref = buffer.at[(zs,) + index]
        return remote(ref, ref, ss.at[zs, 0 if up else 1], rs.at[zs], gy=jnp.clip(z + (1 if up else -1), 0, ny - 1))

    def bx_line(zs, up):
        return line(bxb, s_bxz, r_bxz, zs, up, (c,))

    def by_full(zs, t):
        ref = byb.at[zs, p ^ t]
        return remote(ref, ref, s_byf.at[zs, t], r_byf.at[zs, t], gy=jnp.where(low, z + 1, z - 1))

    def by_cross(zs):
        ref = byb.at[zs, p]
        return remote(ref, ref, s_byc.at[zs], r_byc.at[zs], gy=jnp.where(low, mid, mid - 1))

    def across(j):
        return jnp.where(low, mid + j, mid - 1 - j)

    def outside(j):
        return jnp.where(low, z - 1 - j, z + 1 + j)

    def is_outside(j):
        return jnp.where(low, z - 1 - j >= 0, z + 1 + j < ny)

    def goes_on(up):
        return z + 1 < ny if up else z > 0

    def source(r, up):
        zs = z - r if up else z + r
        return zs, jnp.logical_and(zs >= 0, zs < ny)

    def bx_pass(zs):
        return remote(bxb.at[zs, c], bxb.at[zs, c], s_bxd.at[zs], r_bxd.at[zs], gz=other)

    def piece(zs, owner, part):
        return byb.at[zs, owner, pl.ds(part * half, half), :]

    def plane_direct(zs, t):
        slot = 0 if t == 1 else t
        copies = []
        for n, part in enumerate((0, 1) if t == 1 else (1, 0)):
            ref = piece(zs, p, part)
            copies.append(remote(ref, ref, s_byp.at[zs, slot + n], r_byp.at[zs, t, part], gx=p ^ t))
        return copies

    def relay_xy(zs, b):
        ref = piece(zs, p ^ 1, 0)
        return remote(ref, ref, s_byp.at[zs, 2 * nb + b - 1], r_byp.at[zs, 2 * b + 1, 0], gx=p ^ (2 * b))

    def relay_yx(zs, b):
        ref = piece(zs, p ^ (2 * b), 1)
        return remote(ref, ref, s_byp.at[zs, 3 * nb + b - 2], r_byp.at[zs, 2 * b + 1, 1], gx=p ^ 1)

    def wait_piece(zs, t, part):
        ref = piece(zs, p ^ t, part)
        remote(ref, ref, s_byp.at[zs, 0], r_byp.at[zs, t, part], gx=p ^ 1).wait_recv()

    def pass_xy(zs):
        wait_piece(zs, 1, 0)
        for b in range(1, nb):
            relay_xy(zs, b).start()

    def pass_yx(zs):
        for b in range(1, nb):
            wait_piece(zs, 2 * b, 1)
            relay_yx(zs, b).start()

    def plane_y(zs):
        for b in range(1, nb):
            for copy in plane_direct(zs, 2 * b):
                copy.start()

    def plane_x(zs):
        for copy in plane_direct(zs, 1):
            copy.start()

    def g_copies(zs):
        return [
            remote(gs.at[zs, py ^ b], grecv.at[zs, b - 1], s_g.at[zs, b - 1], r_g.at[zs, b - 1], gx=p ^ (2 * b))
            for b in range(1, nb)
        ]

    def first(zs):
        bx_pass_in(zs).wait_recv()

        def tile(i):
            cc, n = i // (yb // yq), i % (yb // yq)
            part = contract(bxb[zs, cc], wide[:, cols(n * yq, yq)], (0, 0)).astype(BF16)
            for b in range(nb):
                gs[zs, b, cc, :, cols(n * yq, yq)] = part[b * ib : (b + 1) * ib]

        loop(2 * (yb // yq), tile)
        for copy in g_copies(zs):
            copy.start()

    def bx_pass_in(zs):
        return remote(bxb.at[zs, other], bxb.at[zs, other], s_bxd.at[zs], r_bxd.at[zs], gz=other)

    def home(zs):
        return jnp.where(zs < mid, mid - 1, mid)

    def g_send(zs):
        return remote(gs.at[zs, py], gall.at[z, c, zs % mid], s_ga.at[zs], r_ga.at[z, zs % mid], gy=home(zs))

    def g_pass(zs, core, blk):
        ref = gall.at[zs, core, blk]
        return remote(ref, ref, s_gd.at[zs, blk], r_gd.at[zs, blk], gz=other)

    def collect(zs):
        for copy in g_copies(zs):
            copy.wait_recv()

        def tile(i):
            cc, n = i // (yb // yq), i % (yb // yq)
            lanes = cols(n * yq, yq)
            total = gs[zs, py, cc, :, lanes].astype(F32)
            for b in range(1, nb):
                total = total + grecv[zs, b - 1, cc, :, lanes].astype(F32)

            @pl.when(home(zs) != z)
            def _():
                gs[zs, py, cc, :, lanes] = total.astype(BF16)

            @pl.when(home(zs) == z)
            def _():
                gall[z, c, zs % mid, cc, :, lanes] = total.astype(BF16)

        loop(2 * (yb // yq), tile)

        @pl.when(home(zs) != z)
        def _():
            g_send(zs).start()

        @pl.when(home(zs) == z)
        def _():
            g_pass(z, c, zs % mid).start()

    def both(r, act):
        for up in (True, False):
            zs, valid = source(r, up)

            @pl.when(valid)
            def _(zs=zs, up=up):
                act(zs, up)

    def onward(maker, zs, up):
        @pl.when(goes_on(up))
        def _():
            maker(zs, up).start()

    def each(r, act):
        for up in (True, False):
            zs, valid = source(r, up)
            valid = jnp.logical_and(valid, r >= 0 if up else r > 0)

            @pl.when(valid)
            def _(zs=zs):
                act(zs)

    def bx_step(zs, up):
        bx_line(zs, up).wait_recv()
        onward(bx_line, zs, up)
        bx_pass(zs).start()

    def crossing(j):
        zs = across(j)
        by_cross(zs).wait_recv()
        plane_y(zs)
        plane_x(zs)

    def cross_outside(j):
        def act():
            by_full(outside(j), 0).wait_recv()
            by_cross(outside(j)).start()

        when(is_outside(j), act)

    def inward(j):
        def act():
            for t in range(nx):
                by_full(outside(j), t).wait_recv()
                by_full(outside(j), t).start()

        when(is_outside(j), act)

    def own_y_inward():
        for b in range(1, nb):
            wait_piece(z, 2 * b, 0)
            by_full(z, 2 * b).start()

    def own_x_inward():
        wait_piece(z, 1, 1)
        by_full(z, 1).start()

    def own_rest_inward():
        for b in range(1, nb):
            wait_piece(z, 2 * b + 1, 0)
            wait_piece(z, 2 * b + 1, 1)
            by_full(z, 2 * b + 1).start()

    def far_relays(j):
        pass_yx(across(j))
        pass_xy(across(j))

    def round_of(i):
        r = i + 1
        both(r, bx_step)

        @pl.when(r == 1)
        def _():
            when(works, lambda: loop(mid - 1, cross_outside))
            remote(wide.at[theirs, :], wide.at[theirs, :], s_head.at[1], r_head.at[1], gx=p ^ 1).wait_recv()
            first(z)

        each(r, first)

        @pl.when(r == 2)
        def _():
            pass_xy(z)
            each(0, collect)
            when(rests, own_x_inward)
            each(1, collect)
            when(works, lambda: loop(mid - 1, lambda j: crossing(j + 1)))
            if mid > 2:
                when(rests, lambda: loop(mid - 1, inward))

        @pl.when(r == 3)
        def _():
            when(works, lambda: pass_xy(across(0)))

        @pl.when(r > 2)
        def _():
            each(r - 1, collect)

        @pl.when(r == 3)
        def _():
            when(works, lambda: pass_yx(across(0)))
            when(works, lambda: loop(mid - 1, lambda j: far_relays(j + 1)))

        @pl.when(r == 4)
        def _():
            when(rests, own_rest_inward)

    local[0].wait()
    when(works, lambda: by_cross(z).start())
    when(rests, lambda: by_full(z, 0).start())
    plane_y(z)
    local[1].wait()
    swap_rhs.start()
    plane_x(z)
    for copy in local[2:]:
        copy.wait()
    ezall[c] = jnp.broadcast_to(ez[...], (8, LANES))
    for copy in eigs:
        copy.start()
    remote(bx.at[:, cols(px * ci, ci)], bxb.at[z, c, theirs, :], s_head.at[0], r_head.at[0], gx=p ^ 1).wait_recv()
    both(0, lambda zs, up: onward(bx_line, zs, up))
    bx_pass(z).start()

    @pl.when(works)
    def _():
        crossing(0)

    pass_yx(z)
    when(rests, own_y_inward)
    loop(max(ny, 4), round_of)

    for t in range(1, nx):
        remote(exall.at[p ^ t], exall.at[p ^ t], s_eig.at[t], r_eig.at[t], gx=p ^ t).wait_recv()
    for d in range(1, ny):
        far = (z - d) % ny
        remote(eyall.at[far], eyall.at[far], s_eig.at[nx + d], r_eig.at[nx + d], gy=(z + d) % ny).wait_recv()
    remote(ezall.at[other], ezall.at[other], s_eig.at[0], r_eig.at[0], gz=other).wait_recv()
    for blk in range(mid):
        for cc in range(2):
            start = ((place * mid + blk) * 2 + cc) * cx + px * ci + py * ib
            line_at = start // LANES
            per = xb // LANES
            row = exall[line_at // per, pl.ds(line_at % per, 1), :]
            lane = lax.broadcasted_iota(jnp.int32, (ib, LANES), 1)
            want = lax.broadcasted_iota(jnp.int32, (ib, LANES), 0) + start % LANES
            column = jnp.sum(jnp.where(lane == want, jnp.broadcast_to(row, (ib, LANES)), 0.0), axis=1, keepdims=True)
            for k in range(2):
                dcol[k, pl.ds((blk * 2 + cc) * ib, ib), :] = jnp.broadcast_to(column, (ib, LANES)) + ezall[k, 0:1, :]

    def arrive(i):
        zs, blk = (z + 1 + i // mid) % ny, i % mid
        remote(gall.at[zs, c, blk], gall.at[zs, c, blk], s_ga.at[zs], r_ga.at[zs, blk], gy=zs).wait_recv()
        g_pass(zs, c, blk).start()

    def passed(i):
        g_pass(i // mid, other, i % mid).wait_recv()

    @pl.when(works)
    def _():
        loop((ny - 1) * mid, arrive)
        loop(ny * mid, passed)

    eacc[...] = jnp.zeros_like(eacc)

    tn = min(cy, 256)
    ni = 2 * mid * ib

    def second(t):
        owner = p ^ t

        def landed(zs):
            outer = jnp.logical_and((zs < mid) == low, zs != z)

            @pl.when(jnp.logical_and(outer, t > 0))
            def _():
                by_full(zs, t).wait_recv()

            @pl.when(jnp.logical_and(jnp.logical_not(outer), t % 2 == 1))
            def _():
                wait_piece(zs, t, 1)

            @pl.when(jnp.logical_and(jnp.logical_not(outer), t > 1))
            def _():
                wait_piece(zs, t, 0)

        loop(ny, landed)

        def tile(i):
            n, k = i // 2, i % 2
            h = None
            for zs in range(ny):
                term = contract(gall[zs, k].reshape(ni, yb), byb[zs, owner, :, cols(n * tn, tn)], (1, 0))
                h = term if h is None else h + term
            for l in range(tn // LANES):
                line_at = ((owner * 2 + c) * cy + n * tn) // LANES + l
                per = yb // LANES
                row = eyall[line_at // per, pl.ds(line_at % per, 1), :]
                part = h[:, l * LANES : (l + 1) * LANES]
                w = part / (dcol[k] + row)
                eacc[...] += jnp.sum((part * w).reshape(-1, 8, LANES), axis=0)
                wbuf[owner, k, :, cols(n * tn + l * LANES, LANES)] = w.astype(BF16)

        loop(2 * (cy // tn), tile)

    when(works, lambda: loop(nx, second))

    def v_pass(q, zs, core):
        lanes = cols(q * yq, yq)
        return remote(
            gall.at[zs, core, :, :, :, lanes], vrecv.at[zs, :, :, :, lanes], s_vd.at[q, zs], r_vd.at[q, zs], gz=other
        )

    def v_slot(q, side, owner):
        return vfull.at[q, pl.ds(side * mid, mid), :, pl.ds(pl.multiple_of(owner * ib, ib), ib), :]

    def v_send(q, zs):
        return remote(
            gall.at[zs, c, :, :, :, cols(q * yq, yq)], v_slot(q, place, py), s_va.at[q, zs], r_va.at[q, place], gy=zs
        )

    def v_copies(q, side):
        slot = v_slot(q, side, py)
        return [
            remote(slot, slot, s_vb.at[q, side, b - 1], r_vb.at[q, side, b - 1], gx=p ^ (2 * b)) for b in range(1, nb)
        ]

    def target_of(d):
        end = jnp.where(d % 2 == 0, ny - 1 - d // 2, d // 2)
        return jnp.where(low, end, ny - 1 - end)

    def third(q, d):
        zs = target_of(d)

        def mode(i):
            k = jnp.where(i == 0, other, c)
            v = None
            for owner in range(nx):
                term = contract(wbuf[owner, k], byb[zs, owner, rows(q * yq, yq), :], (1, 1))
                v = term if v is None else v + term
            gall[zs, k, :, :, :, cols(q * yq, yq)] = v.astype(BF16).reshape(mid, 2, ib, yq)
            when(i == 0, lambda: v_pass(q, zs, other).start())

        loop(2, mode)

    def merge(q, d):
        zs = target_of(d)
        lanes = cols(q * yq, yq)
        v_pass(q, zs, c).wait_recv()
        v = (gall[zs, c, :, :, :, lanes].astype(F32) + vrecv[zs, :, :, :, lanes].astype(F32)).astype(BF16)

        @pl.when(zs != z)
        def _():
            gall[zs, c, :, :, :, lanes] = v
            v_send(q, zs).start()

        @pl.when(zs == z)
        def _():
            vfull[q, pl.ds(place * mid, mid), :, pl.ds(pl.multiple_of(py * ib, ib), ib), :] = v
            for copy in v_copies(q, place):
                copy.start()

    def spread(q):
        def target(i):
            side = jnp.where(low, i, 1 - i)

            @pl.when(mid - 1 + side != z)
            def _():
                slot = v_slot(q, side, py)
                remote(slot, slot, s_va.at[q, 0], r_va.at[q, side], gy=(z + 1) % ny).wait_recv()
                for copy in v_copies(q, side):
                    copy.start()

        loop(2, target)

    mt = min(xb, 512)

    def s_copy(q):
        lanes = cols(q * yq, yq)
        return remote(wide.at[theirs, lanes], srecv.at[:, lanes], s_s.at[q], r_s.at[q], gx=p ^ 1)

    def fourth(q):
        lanes = cols(q * yq, yq)

        def landed(side):
            for b in range(1, nb):
                slot = v_slot(q, side, py ^ b)
                remote(slot, slot, s_vb.at[q, side, b - 1], r_vb.at[q, side, b - 1], gx=p ^ (2 * b)).wait_recv()

        loop(2, landed)

        def tile(i):
            m, own = i % (xb // mt), i // (xb // mt)
            side = jnp.where(own == 1, px, 1 - px)
            at = rows(side * xb + m * mt, mt)
            s = None
            for zs in range(ny):
                for cc in range(2):
                    term = contract(bxb[zs, cc, at, :], vfull[q, zs, cc], (1, 0))
                    s = term if s is None else s + term

            @pl.when(own == 0)
            def _():
                wide[at, lanes] = s.astype(BF16)

                @pl.when(m == xb // mt - 1)
                def _():
                    s_copy(q).start()

            @pl.when(own == 1)
            def _():
                sown[rows(m * mt, mt), lanes] = s

        loop(2 * (xb // mt), tile)

    def out_copy(q):
        lanes = cols(q * yq, yq)
        return pltpu.make_async_copy(wide.at[mine, lanes], out.at[0, :, lanes], s_out.at[q])

    def finish(q):
        lanes = cols(q * yq, yq)
        s_copy(q).wait_recv()

        def tile(m):
            at = rows(m * mt, mt)
            wide[rows(px * xb + m * mt, mt), lanes] = (sown[at, lanes] + srecv[at, lanes].astype(F32)).astype(BF16)

        loop(xb // mt, tile)
        out_copy(q).start()

    def left(i):
        g_pass(i // mid, c, i % mid).wait_send()

    when(works, lambda: loop(ny * mid, left))
    swap_rhs.wait_send()

    e_core = remote(eacc, e1, s_e.at[0], r_e.at[0], gz=other)
    e_plane = [remote(e2.at[p], e2.at[p], s_e.at[t], r_e.at[t], gx=p ^ t) for t in range(1, nx)]
    e_line = [remote(e3.at[place], e3.at[place], s_e.at[nx + d], r_e.at[nx + place], gy=(z + d) % ny) for d in range(1, ny)]

    def leave(q):
        def step(d):
            start = q == 0

            @pl.when(jnp.logical_and(start, d == 0))
            def _():
                e_core.start()

            @pl.when(jnp.logical_and(start, d == 2))
            def _():
                e_core.wait_recv()
                e2[p] = eacc[...] + e1[...]
                for copy in e_plane:
                    copy.start()

            @pl.when(jnp.logical_and(start, d == ny + 1))
            def _():
                for s in range(1, nx):
                    remote(e2.at[p ^ s], e2.at[p ^ s], s_e.at[s], r_e.at[s], gx=p ^ s).wait_recv()
                total = e2[0]
                for s in range(1, nx):
                    total = total + e2[s]
                e3[place] = total
                for copy in e_line:
                    copy.start()

            @pl.when(d < ny)
            def _():
                third(q, d)

            @pl.when(d >= 2)
            def _():
                merge(q, d - 2)

        loop(ny + 2, step)

    def stage(t, lag, act):
        @pl.when(jnp.logical_and(t >= lag, t < chunks + lag))
        def _():
            act(t - lag)

    def tail(t):
        stage(t, 0, lambda q: when(works, lambda: leave(q)))
        stage(t, 1, spread)
        stage(t, 2, fourth)
        stage(t, 3, finish)

    loop(chunks + 3, tail)

    for side in range(2):
        @pl.when(mid - 1 + side != z)
        def _(side=side):
            remote(e3.at[side], e3.at[side], s_e.at[0], r_e.at[nx + side], gy=(z + 1) % ny).wait_recv()

    total = e3[0] + e3[1]
    energy[0] = jnp.sum(total)

    swap_bx.wait_send()
    for copy in eigs:
        copy.wait_send()

    @pl.when(works)
    def _():
        for copy in [e_core] + e_plane + e_line:
            copy.wait_send()

    def plane_drain(zs):
        for t in [1] + [2 * b for b in range(1, nb)]:
            for copy in plane_direct(zs, t):
                copy.wait_send()
        for b in range(1, nb):
            relay_xy(zs, b).wait_send()
            relay_yx(zs, b).wait_send()

    def drain(zs):
        for up in (True, False):
            from_here = zs <= z if up else zs >= z

            @pl.when(jnp.logical_and(goes_on(up), from_here))
            def _(up=up):
                bx_line(zs, up).wait_send()

        bx_pass(zs).wait_send()
        for copy in g_copies(zs):
            copy.wait_send()
        same = (zs < mid) == low
        when(jnp.logical_or(zs == z, jnp.logical_and(works, jnp.logical_not(same))), lambda: plane_drain(zs))
        when(jnp.logical_and(works, same), lambda: by_cross(zs).wait_send())

        @pl.when(jnp.logical_and(jnp.logical_and(jnp.logical_not(works), same), jnp.where(low, zs <= z, zs >= z)))
        def _():
            for t in range(nx):
                by_full(zs, t).wait_send()

        when(home(zs) != z, lambda: g_send(zs).wait_send())

        @pl.when(works)
        def _():
            def chunk(q):
                v_pass(q, zs, other).wait_send()
                when(zs != z, lambda: v_send(q, zs).wait_send())

            loop(chunks, chunk)

    loop(ny, drain)

    def drain_chunk(q):
        s_copy(q).wait_send()
        out_copy(q).wait()
        for side in range(2):
            for copy in v_copies(q, side):
                copy.wait_send()

    loop(chunks, drain_chunk)


def shards(nx, ny, rhs, basis_x, basis_y, eig_x, eig_y, eig_z):
    xb, yb = rhs.shape[1], rhs.shape[2]
    cx, cy = basis_x.shape[1], basis_y.shape[1]
    nb, ci = nx // 2, cx // 2
    ib = ci // nb
    yq = min(yb, 256)
    chunks, mid = yb // yq, ny // 2
    ex = eig_x.reshape(xb // LANES, LANES)
    ey = eig_y.reshape(yb // LANES, LANES)
    ez = eig_z.reshape(1, 1)
    dma = pltpu.SemaphoreType.DMA
    any_space, vmem = pl.BlockSpec(memory_space=pl.ANY), pl.BlockSpec(memory_space=pltpu.VMEM)
    solution, energy = pl.pallas_call(
        functools.partial(kernel, nx, ny, yq),
        name="solve",
        out_shape=(
            jax.ShapeDtypeStruct(rhs.shape, BF16),
            jax.ShapeDtypeStruct((1,), F32),
        ),
        in_specs=[any_space] * 3 + [vmem] * 3,
        out_specs=(any_space, pl.BlockSpec(memory_space=pltpu.SMEM)),
        scratch_shapes=[
            pltpu.VMEM((ny, 2, 2 * xb, ci), BF16),
            pltpu.VMEM((ny, nx, yb, cy), BF16),
            pltpu.VMEM((2 * xb, yb), BF16),
            pltpu.VMEM((ny, nb, 2, ib, yb), BF16),
            pltpu.VMEM((ny, nb - 1, 2, ib, yb), BF16),
            pltpu.VMEM((ny, 2, mid, 2, ib, yb), BF16),
            pltpu.VMEM((nx, 2, 2 * mid * ib, cy), BF16),
            pltpu.VMEM((ny, mid, 2, ib, yb), BF16),
            pltpu.VMEM((chunks, ny, 2, nb * ib, yq), BF16),
            pltpu.VMEM((xb, yb), F32),
            pltpu.VMEM((xb, yb), BF16),
            pltpu.VMEM((nx, xb // LANES, LANES), F32),
            pltpu.VMEM((ny, yb // LANES, LANES), F32),
            pltpu.VMEM((2, 8, LANES), F32),
            pltpu.VMEM((2, 2 * mid * ib, LANES), F32),
            pltpu.VMEM((8, LANES), F32),
            pltpu.VMEM((8, LANES), F32),
            pltpu.VMEM((nx, 8, LANES), F32),
            pltpu.VMEM((2, 8, LANES), F32),
            dma((5,)),
            dma((nx + ny,)), dma((nx + ny,)),
            dma((2,)), dma((2,)),
            dma((ny, 2)), dma((ny,)),
            dma((ny,)), dma((ny,)),
            dma((ny, nx)), dma((ny, nx)),
            dma((ny,)), dma((ny,)),
            dma((ny, 4 * nb - 2)), dma((ny, nx, 2)),
            dma((ny, nb - 1)), dma((ny, nb - 1)),
            dma((ny,)), dma((ny, mid)),
            dma((ny, mid)), dma((ny, mid)),
            dma((chunks, ny)), dma((chunks, ny)),
            dma((chunks, ny)), dma((chunks, 2)),
            dma((chunks, 2, nb - 1)), dma((chunks, 2, nb - 1)),
            dma((chunks,)), dma((chunks,)),
            dma((chunks,)),
            dma((nx + ny,)), dma((nx + ny,)),
        ],
        compiler_params=pltpu.CompilerParams(
            collective_id=0, has_side_effects=True, vmem_limit_bytes=65472 * 1024
        ),
    )(rhs, basis_x, basis_y, ex, ey, ez)
    return solution, energy.reshape(())


def solution(mesh):
    return jax.shard_map(
        functools.partial(shards, mesh.shape["gx"], mesh.shape["gy"]),
        mesh=mesh,
        in_specs=(
            P("gz", "gx", "gy"),
            P("gx", ("gy", "gz")),
            P("gy", ("gx", "gz")),
            P("gx"),
            P("gy"),
            P("gz"),
        ),
        out_specs=(P("gz", "gx", "gy"), P()),
        check_vma=False,
    )
```

```python
import functools

import jax
import jax.numpy as jnp
from jax import lax
from jax.experimental import pallas as pl
from jax.experimental.pallas import tpu as pltpu
from jax.sharding import PartitionSpec as P

BF16, F32 = jnp.bfloat16, jnp.float32
LANES = 128


def contract(left, right, dims):
    return lax.dot_general(left, right, ((dims[:1], dims[1:]), ((), ())), preferred_element_type=F32)


def kernel(
    nx, ny, yq,
    rhs, bx, by, ex, ey, ez,
    out, energy,
    bxb, byb, wide, gs, grecv, gall, wbuf, vrecv, vfull, sown, srecv,
    exall, eyall, ezall, dcol, eacc, e1, e2, e3,
    s_loc, s_eig, r_eig, s_head, r_head, s_bxz, r_bxz, s_bxd, r_bxd, s_byf, r_byf, s_byc, r_byc, s_byp, r_byp,
    s_g, r_g, s_ga, r_ga, s_gd, r_gd, s_vd, r_vd, s_va, r_va, s_vb, r_vb, s_s, r_s, s_out, s_e, r_e,
):
    p, z, c = lax.axis_index("gx"), lax.axis_index("gy"), lax.axis_index("gz")
    px, py = p % 2, p // 2
    nb = nx // 2
    xb, yb = rhs.shape[1], rhs.shape[2]
    cx, cy = bx.shape[1], by.shape[1]
    ci = cx // 2
    ib = ci // nb
    chunks = yb // yq
    half = yb // 2
    other = 1 - c
    mid = ny // 2
    low = z < mid
    works = jnp.logical_or(z == mid - 1, z == mid)
    rests = jnp.logical_not(works)
    place = jnp.where(low, 0, 1)

    def when(condition, act):
        @pl.when(condition)
        def _():
            act()

    def remote(src, dst, ss, rs, **where):
        return pltpu.make_async_remote_copy(
            src_ref=src, dst_ref=dst, send_sem=ss, recv_sem=rs,
            device_id=where, device_id_type=pl.DeviceIdType.MESH,
        )

    def loop(count, body):
        lax.fori_loop(0, count, lambda i, carry: (body(i), carry)[1], 0)

    def cols(start, size):
        return pl.ds(pl.multiple_of(start, LANES), size)

    def rows(start, size):
        return pl.ds(pl.multiple_of(start, size), size)

    barrier = pltpu.get_barrier_semaphore()
    for t in range(1, nx):
        pl.semaphore_signal(barrier, inc=1, device_id={"gx": p ^ t}, device_id_type=pl.DeviceIdType.MESH)
    for d in range(1, ny):
        pl.semaphore_signal(barrier, inc=1, device_id={"gy": (z + d) % ny}, device_id_type=pl.DeviceIdType.MESH)
    pl.semaphore_signal(barrier, inc=1, device_id={"gz": other}, device_id_type=pl.DeviceIdType.MESH)

    mine = rows(px * xb, xb)
    theirs = rows((1 - px) * xb, xb)
    local = [
        pltpu.make_async_copy(by, byb.at[z, p], s_loc.at[0]),
        pltpu.make_async_copy(rhs.at[0], wide.at[mine, :], s_loc.at[1]),
        pltpu.make_async_copy(bx.at[:, cols(px * ci, ci)], bxb.at[z, c, mine, :], s_loc.at[2]),
        pltpu.make_async_copy(ex, exall.at[p], s_loc.at[3]),
        pltpu.make_async_copy(ey, eyall.at[z], s_loc.at[4]),
    ]
    for copy in local:
        copy.start()
    pl.semaphore_wait(barrier, nx + ny - 1)

    swap_bx = remote(bx.at[:, cols((1 - px) * ci, ci)], bxb.at[z, c, mine, :], s_head.at[0], r_head.at[0], gx=p ^ 1)
    swap_bx.start()
    wing = yb // 2

    def swap_rhs(side, part):
        ref = wide.at[side, pl.ds(part * wing, wing)]
        return remote(ref, ref, s_head.at[1 + part], r_head.at[1 + part], gx=p ^ 1)

    eigs = [remote(exall.at[p], exall.at[p], s_eig.at[t], r_eig.at[t], gx=p ^ t) for t in range(1, nx)]
    eigs += [
        remote(eyall.at[z], eyall.at[z], s_eig.at[nx + d], r_eig.at[nx + d], gy=(z + d) % ny) for d in range(1, ny)
    ]
    eigs += [remote(ezall.at[c], ezall.at[c], s_eig.at[0], r_eig.at[0], gz=other)]

    def line(buffer, ss, rs, zs, up, index):
        ref = buffer.at[(zs,) + index]
        return remote(ref, ref, ss.at[zs, 0 if up else 1], rs.at[zs], gy=jnp.clip(z + (1 if up else -1), 0, ny - 1))

    def bx_line(zs, up):
        return line(bxb, s_bxz, r_bxz, zs, up, (c,))

    def by_full(zs, t, part):
        ref = piece(zs, p ^ t, part)
        return remote(
            ref, ref, s_byf.at[zs, t, part], r_byf.at[zs, t, part], gy=jnp.where(low, z + 1, z - 1)
        )

    def by_cross(zs):
        ref = byb.at[zs, p]
        return remote(ref, ref, s_byc.at[zs], r_byc.at[zs], gy=jnp.where(low, mid, mid - 1))

    def across(j):
        return jnp.where(low, mid + j, mid - 1 - j)

    def outside(j):
        return jnp.where(low, z - 1 - j, z + 1 + j)

    def is_outside(j):
        return jnp.where(low, z - 1 - j >= 0, z + 1 + j < ny)

    def goes_on(up):
        return z + 1 < ny if up else z > 0

    def source(r, up):
        zs = z - r if up else z + r
        return zs, jnp.logical_and(zs >= 0, zs < ny)

    def bx_pass(zs):
        return remote(bxb.at[zs, c], bxb.at[zs, c], s_bxd.at[zs], r_bxd.at[zs], gz=other)

    def piece(zs, owner, part):
        return byb.at[zs, owner, pl.ds(part * half, half), :]

    def plane_direct(zs, t):
        slot = 0 if t == 1 else t
        copies = []
        for n, part in enumerate((0, 1) if t == 1 else (1, 0)):
            ref = piece(zs, p, part)
            copies.append(remote(ref, ref, s_byp.at[zs, slot + n], r_byp.at[zs, t, part], gx=p ^ t))
        return copies

    def relay_xy(zs, b):
        ref = piece(zs, p ^ 1, 0)
        return remote(ref, ref, s_byp.at[zs, 2 * nb + b - 1], r_byp.at[zs, 2 * b + 1, 0], gx=p ^ (2 * b))

    def relay_yx(zs, b):
        ref = piece(zs, p ^ (2 * b), 1)
        return remote(ref, ref, s_byp.at[zs, 3 * nb + b - 2], r_byp.at[zs, 2 * b + 1, 1], gx=p ^ 1)

    def wait_piece(zs, t, part):
        ref = piece(zs, p ^ t, part)
        remote(ref, ref, s_byp.at[zs, 0], r_byp.at[zs, t, part], gx=p ^ 1).wait_recv()

    def pass_xy(zs):
        wait_piece(zs, 1, 0)
        for b in range(1, nb):
            relay_xy(zs, b).start()

    def pass_yx(zs):
        for b in range(1, nb):
            wait_piece(zs, 2 * b, 1)
            relay_yx(zs, b).start()

    def plane_y(zs):
        for b in range(1, nb):
            for copy in plane_direct(zs, 2 * b):
                copy.start()

    def plane_x(zs):
        for copy in plane_direct(zs, 1):
            copy.start()

    def g_copies(zs, part):
        lanes = pl.ds(part * wing, wing)
        return [
            remote(
                gs.at[zs, py ^ b, :, :, lanes], grecv.at[zs, b - 1, :, :, lanes],
                s_g.at[zs, part, b - 1], r_g.at[zs, part, b - 1], gx=p ^ (2 * b),
            )
            for b in range(1, nb)
        ]

    def first(zs, part):
        def tile(i):
            cc, n = i // (wing // yq), i % (wing // yq)
            lanes = cols(part * wing + n * yq, yq)
            sums = contract(bxb[zs, cc], wide[:, lanes], (0, 0)).astype(BF16)
            for b in range(nb):
                gs[zs, b, cc, :, lanes] = sums[b * ib : (b + 1) * ib]

        loop(2 * (wing // yq), tile)
        for copy in g_copies(zs, part):
            copy.start()

    def first_whole(zs):
        bx_pass_in(zs).wait_recv()
        first(zs, 0)
        first(zs, 1)

    def first_left(zs):
        bx_pass_in(zs).wait_recv()
        first(zs, 0)

    def first_right(zs):
        first(zs, 1)

    def bx_pass_in(zs):
        return remote(bxb.at[zs, other], bxb.at[zs, other], s_bxd.at[zs], r_bxd.at[zs], gz=other)

    def home(zs):
        return jnp.where(zs < mid, mid - 1, mid)

    def g_send(zs):
        return remote(gs.at[zs, py], gall.at[z, c, zs % mid], s_ga.at[zs], r_ga.at[z, zs % mid], gy=home(zs))

    def g_pass(zs, core, blk):
        ref = gall.at[zs, core, blk]
        return remote(ref, ref, s_gd.at[zs, blk], r_gd.at[zs, blk], gz=other)

    def collect(zs):
        for part in range(2):
            for copy in g_copies(zs, part):
                copy.wait_recv()

        def tile(i):
            cc, n = i // (yb // yq), i % (yb // yq)
            lanes = cols(n * yq, yq)
            total = gs[zs, py, cc, :, lanes].astype(F32)
            for b in range(1, nb):
                total = total + grecv[zs, b - 1, cc, :, lanes].astype(F32)

            @pl.when(home(zs) != z)
            def _():
                gs[zs, py, cc, :, lanes] = total.astype(BF16)

            @pl.when(home(zs) == z)
            def _():
                gall[z, c, zs % mid, cc, :, lanes] = total.astype(BF16)

        loop(2 * (yb // yq), tile)

        @pl.when(home(zs) != z)
        def _():
            g_send(zs).start()

        @pl.when(home(zs) == z)
        def _():
            g_pass(z, c, zs % mid).start()

    def both(r, act):
        for up in (True, False):
            zs, valid = source(r, up)

            @pl.when(valid)
            def _(zs=zs, up=up):
                act(zs, up)

    def onward(maker, zs, up):
        @pl.when(goes_on(up))
        def _():
            maker(zs, up).start()

    def each(r, act):
        for up in (True, False):
            zs, valid = source(r, up)
            valid = jnp.logical_and(valid, r >= 0 if up else r > 0)

            @pl.when(valid)
            def _(zs=zs):
                act(zs)

    def bx_step(zs, up):
        bx_line(zs, up).wait_recv()
        onward(bx_line, zs, up)
        bx_pass(zs).start()

    def crossing(j):
        zs = across(j)
        by_cross(zs).wait_recv()
        plane_y(zs)
        plane_x(zs)

    def cross_outside(j):
        def act():
            for part in range(2):
                by_full(outside(j), 0, part).wait_recv()
            by_cross(outside(j)).start()

        when(is_outside(j), act)

    def inward(j):
        def act():
            for t in range(nx):
                for part in range(2):
                    by_full(outside(j), t, part).wait_recv()
                    by_full(outside(j), t, part).start()

        when(is_outside(j), act)

    def own_y_inward():
        for b in range(1, nb):
            by_full(z, 2 * b, 1).start()
            wait_piece(z, 2 * b, 0)
            by_full(z, 2 * b, 0).start()

    def own_x_inward():
        wait_piece(z, 1, 1)
        by_full(z, 1, 1).start()

    def own_rest_inward():
        for b in range(1, nb):
            for part in range(2):
                wait_piece(z, 2 * b + 1, part)
                by_full(z, 2 * b + 1, part).start()

    def far_relays(j):
        pass_yx(across(j))
        pass_xy(across(j))

    def round_of(i):
        r = i + 1
        both(r, bx_step)

        @pl.when(r == 1)
        def _():
            when(works, lambda: loop(mid - 1, cross_outside))
            each(1, first_left)
            swap_rhs(theirs, 1).wait_recv()
            first(z, 1)
            each(1, first_right)

        @pl.when(r == 2)
        def _():
            pass_xy(z)
            when(rests, lambda: by_full(z, 1, 0).start())

        @pl.when(r > 1)
        def _():
            each(r, first_whole)

        @pl.when(r == 2)
        def _():
            each(0, collect)
            each(1, collect)
            when(works, lambda: loop(mid - 1, lambda j: crossing(j + 1)))
            if mid > 2:
                when(rests, lambda: loop(mid - 1, inward))

        @pl.when(r == 3)
        def _():
            when(works, lambda: pass_xy(across(0)))

        @pl.when(r > 2)
        def _():
            each(r - 1, collect)

        @pl.when(r == 3)
        def _():
            when(works, lambda: pass_yx(across(0)))
            when(works, lambda: loop(mid - 1, lambda j: far_relays(j + 1)))

        @pl.when(r == 4)
        def _():
            when(rests, own_x_inward)
            when(rests, own_rest_inward)

    local[0].wait()
    when(works, lambda: by_cross(z).start())
    for part in range(2):
        when(rests, lambda part=part: by_full(z, 0, part).start())
    plane_y(z)
    local[1].wait()
    swap_rhs(mine, 0).start()
    swap_rhs(mine, 1).start()
    plane_x(z)
    for copy in local[2:]:
        copy.wait()
    ezall[c] = jnp.broadcast_to(ez[...], (8, LANES))
    for copy in eigs:
        copy.start()
    remote(bx.at[:, cols(px * ci, ci)], bxb.at[z, c, theirs, :], s_head.at[0], r_head.at[0], gx=p ^ 1).wait_recv()
    both(0, lambda zs, up: onward(bx_line, zs, up))
    bx_pass(z).start()

    @pl.when(works)
    def _():
        crossing(0)

    pass_yx(z)
    when(rests, own_y_inward)
    swap_rhs(theirs, 0).wait_recv()
    first_left(z)
    loop(max(ny, 4), round_of)

    for t in range(1, nx):
        remote(exall.at[p ^ t], exall.at[p ^ t], s_eig.at[t], r_eig.at[t], gx=p ^ t).wait_recv()
    for d in range(1, ny):
        far = (z - d) % ny
        remote(eyall.at[far], eyall.at[far], s_eig.at[nx + d], r_eig.at[nx + d], gy=(z + d) % ny).wait_recv()
    remote(ezall.at[other], ezall.at[other], s_eig.at[0], r_eig.at[0], gz=other).wait_recv()
    for blk in range(mid):
        for cc in range(2):
            start = ((place * mid + blk) * 2 + cc) * cx + px * ci + py * ib
            line_at = start // LANES
            per = xb // LANES
            row = exall[line_at // per, pl.ds(line_at % per, 1), :]
            lane = lax.broadcasted_iota(jnp.int32, (ib, LANES), 1)
            want = lax.broadcasted_iota(jnp.int32, (ib, LANES), 0) + start % LANES
            column = jnp.sum(jnp.where(lane == want, jnp.broadcast_to(row, (ib, LANES)), 0.0), axis=1, keepdims=True)
            for k in range(2):
                dcol[k, pl.ds((blk * 2 + cc) * ib, ib), :] = jnp.broadcast_to(column, (ib, LANES)) + ezall[k, 0:1, :]

    def arrive(i):
        zs, blk = (z + 1 + i // mid) % ny, i % mid
        remote(gall.at[zs, c, blk], gall.at[zs, c, blk], s_ga.at[zs], r_ga.at[zs, blk], gy=zs).wait_recv()
        g_pass(zs, c, blk).start()

    def passed(i):
        g_pass(i // mid, other, i % mid).wait_recv()

    @pl.when(works)
    def _():
        loop((ny - 1) * mid, arrive)
        loop(ny * mid, passed)

    eacc[...] = jnp.zeros_like(eacc)

    tn = min(cy, 256)
    ni = 2 * mid * ib

    def second(t):
        owner = p ^ t

        def landed(zs):
            outer = jnp.logical_and((zs < mid) == low, zs != z)

            @pl.when(jnp.logical_and(outer, t > 0))
            def _():
                for part in range(2):
                    by_full(zs, t, part).wait_recv()

            @pl.when(jnp.logical_and(jnp.logical_not(outer), t % 2 == 1))
            def _():
                wait_piece(zs, t, 1)

            @pl.when(jnp.logical_and(jnp.logical_not(outer), t > 1))
            def _():
                wait_piece(zs, t, 0)

        loop(ny, landed)

        def tile(i):
            n, k = i // 2, i % 2
            h = None
            for zs in range(ny):
                term = contract(gall[zs, k].reshape(ni, yb), byb[zs, owner, :, cols(n * tn, tn)], (1, 0))
                h = term if h is None else h + term
            for l in range(tn // LANES):
                line_at = ((owner * 2 + c) * cy + n * tn) // LANES + l
                per = yb // LANES
                row = eyall[line_at // per, pl.ds(line_at % per, 1), :]
                part = h[:, l * LANES : (l + 1) * LANES]
                w = part / (dcol[k] + row)
                eacc[...] += jnp.sum((part * w).reshape(-1, 8, LANES), axis=0)
                wbuf[owner, k, :, cols(n * tn + l * LANES, LANES)] = w.astype(BF16)

        loop(2 * (cy // tn), tile)

    when(works, lambda: loop(nx, second))

    def v_pass(q, zs, core):
        lanes = cols(q * yq, yq)
        return remote(
            gall.at[zs, core, :, :, :, lanes], vrecv.at[zs, :, :, :, lanes], s_vd.at[q, zs], r_vd.at[q, zs], gz=other
        )

    def v_slot(q, side, owner):
        return vfull.at[q, pl.ds(side * mid, mid), :, pl.ds(pl.multiple_of(owner * ib, ib), ib), :]

    def v_send(q, zs):
        return remote(
            gall.at[zs, c, :, :, :, cols(q * yq, yq)], v_slot(q, place, py), s_va.at[q, zs], r_va.at[q, place], gy=zs
        )

    def v_copies(q, side):
        slot = v_slot(q, side, py)
        return [
            remote(slot, slot, s_vb.at[q, side, b - 1], r_vb.at[q, side, b - 1], gx=p ^ (2 * b)) for b in range(1, nb)
        ]

    def target_of(d):
        end = jnp.where(d % 2 == 0, ny - 1 - d // 2, d // 2)
        return jnp.where(low, end, ny - 1 - end)

    def third(q, d):
        zs = target_of(d)

        def mode(i):
            k = jnp.where(i == 0, other, c)
            v = None
            for owner in range(nx):
                term = contract(wbuf[owner, k], byb[zs, owner, rows(q * yq, yq), :], (1, 1))
                v = term if v is None else v + term
            gall[zs, k, :, :, :, cols(q * yq, yq)] = v.astype(BF16).reshape(mid, 2, ib, yq)
            when(i == 0, lambda: v_pass(q, zs, other).start())

        loop(2, mode)

    def merge(q, d):
        zs = target_of(d)
        lanes = cols(q * yq, yq)
        v_pass(q, zs, c).wait_recv()
        v = (gall[zs, c, :, :, :, lanes].astype(F32) + vrecv[zs, :, :, :, lanes].astype(F32)).astype(BF16)

        @pl.when(zs != z)
        def _():
            gall[zs, c, :, :, :, lanes] = v
            v_send(q, zs).start()

        @pl.when(zs == z)
        def _():
            vfull[q, pl.ds(place * mid, mid), :, pl.ds(pl.multiple_of(py * ib, ib), ib), :] = v
            for copy in v_copies(q, place):
                copy.start()

    def spread(q):
        def target(i):
            side = jnp.where(low, i, 1 - i)

            @pl.when(mid - 1 + side != z)
            def _():
                slot = v_slot(q, side, py)
                remote(slot, slot, s_va.at[q, 0], r_va.at[q, side], gy=(z + 1) % ny).wait_recv()
                for copy in v_copies(q, side):
                    copy.start()

        loop(2, target)

    mt = min(xb, 512)

    def s_copy(q):
        lanes = cols(q * yq, yq)
        return remote(wide.at[theirs, lanes], srecv.at[:, lanes], s_s.at[q], r_s.at[q], gx=p ^ 1)

    def fourth(q):
        lanes = cols(q * yq, yq)

        def landed(side):
            for b in range(1, nb):
                slot = v_slot(q, side, py ^ b)
                remote(slot, slot, s_vb.at[q, side, b - 1], r_vb.at[q, side, b - 1], gx=p ^ (2 * b)).wait_recv()

        loop(2, landed)

        def tile(i):
            m, own = i % (xb // mt), i // (xb // mt)
            side = jnp.where(own == 1, px, 1 - px)
            at = rows(side * xb + m * mt, mt)
            s = None
            for zs in range(ny):
                for cc in range(2):
                    term = contract(bxb[zs, cc, at, :], vfull[q, zs, cc], (1, 0))
                    s = term if s is None else s + term

            @pl.when(own == 0)
            def _():
                wide[at, lanes] = s.astype(BF16)

                @pl.when(m == xb // mt - 1)
                def _():
                    s_copy(q).start()

            @pl.when(own == 1)
            def _():
                sown[rows(m * mt, mt), lanes] = s

        loop(2 * (xb // mt), tile)

    def out_copy(q):
        lanes = cols(q * yq, yq)
        return pltpu.make_async_copy(wide.at[mine, lanes], out.at[0, :, lanes], s_out.at[q])

    def finish(q):
        lanes = cols(q * yq, yq)
        s_copy(q).wait_recv()

        def tile(m):
            at = rows(m * mt, mt)
            wide[rows(px * xb + m * mt, mt), lanes] = (sown[at, lanes] + srecv[at, lanes].astype(F32)).astype(BF16)

        loop(xb // mt, tile)
        out_copy(q).start()

    def left(i):
        g_pass(i // mid, c, i % mid).wait_send()

    when(works, lambda: loop(ny * mid, left))
    swap_rhs(mine, 0).wait_send()
    swap_rhs(mine, 1).wait_send()

    e_core = remote(eacc, e1, s_e.at[0], r_e.at[0], gz=other)
    e_plane = [remote(e2.at[p], e2.at[p], s_e.at[t], r_e.at[t], gx=p ^ t) for t in range(1, nx)]
    e_line = [remote(e3.at[place], e3.at[place], s_e.at[nx + d], r_e.at[nx + place], gy=(z + d) % ny) for d in range(1, ny)]

    def leave(q):
        def step(d):
            start = q == 0

            @pl.when(jnp.logical_and(start, d == 0))
            def _():
                e_core.start()

            @pl.when(jnp.logical_and(start, d == 2))
            def _():
                e_core.wait_recv()
                e2[p] = eacc[...] + e1[...]
                for copy in e_plane:
                    copy.start()

            @pl.when(jnp.logical_and(start, d == ny + 1))
            def _():
                for s in range(1, nx):
                    remote(e2.at[p ^ s], e2.at[p ^ s], s_e.at[s], r_e.at[s], gx=p ^ s).wait_recv()
                total = e2[0]
                for s in range(1, nx):
                    total = total + e2[s]
                e3[place] = total
                for copy in e_line:
                    copy.start()

            @pl.when(d < ny)
            def _():
                third(q, d)

            @pl.when(jnp.logical_and(start, d >= 2))
            def _():
                merge(q, d - 2)

        loop(ny + 2, step)

    def stage(t, lag, act):
        @pl.when(jnp.logical_and(t >= lag, t < chunks + lag))
        def _():
            act(t - lag)

    def tail(t):
        stage(t, 0, lambda q: when(works, lambda: leave(q)))
        stage(t, 1, spread)

        @pl.when(jnp.logical_and(works, jnp.logical_and(t >= 1, t < chunks)))
        def _():
            loop(ny, lambda d: merge(t, d))

        stage(t, 2, fourth)
        stage(t, 3, finish)

    loop(chunks + 3, tail)

    for side in range(2):
        @pl.when(mid - 1 + side != z)
        def _(side=side):
            remote(e3.at[side], e3.at[side], s_e.at[0], r_e.at[nx + side], gy=(z + 1) % ny).wait_recv()

    total = e3[0] + e3[1]
    energy[0] = jnp.sum(total)

    swap_bx.wait_send()
    for copy in eigs:
        copy.wait_send()

    @pl.when(works)
    def _():
        for copy in [e_core] + e_plane + e_line:
            copy.wait_send()

    def plane_drain(zs):
        for t in [1] + [2 * b for b in range(1, nb)]:
            for copy in plane_direct(zs, t):
                copy.wait_send()
        for b in range(1, nb):
            relay_xy(zs, b).wait_send()
            relay_yx(zs, b).wait_send()

    def drain(zs):
        for up in (True, False):
            from_here = zs <= z if up else zs >= z

            @pl.when(jnp.logical_and(goes_on(up), from_here))
            def _(up=up):
                bx_line(zs, up).wait_send()

        bx_pass(zs).wait_send()
        for part in range(2):
            for copy in g_copies(zs, part):
                copy.wait_send()
        same = (zs < mid) == low
        when(jnp.logical_or(zs == z, jnp.logical_and(works, jnp.logical_not(same))), lambda: plane_drain(zs))
        when(jnp.logical_and(works, same), lambda: by_cross(zs).wait_send())

        @pl.when(jnp.logical_and(jnp.logical_and(jnp.logical_not(works), same), jnp.where(low, zs <= z, zs >= z)))
        def _():
            for t in range(nx):
                for part in range(2):
                    by_full(zs, t, part).wait_send()

        when(home(zs) != z, lambda: g_send(zs).wait_send())

        @pl.when(works)
        def _():
            def chunk(q):
                v_pass(q, zs, other).wait_send()
                when(zs != z, lambda: v_send(q, zs).wait_send())

            loop(chunks, chunk)

    loop(ny, drain)

    def drain_chunk(q):
        s_copy(q).wait_send()
        out_copy(q).wait()
        for side in range(2):
            for copy in v_copies(q, side):
                copy.wait_send()

    loop(chunks, drain_chunk)


def shards(nx, ny, rhs, basis_x, basis_y, eig_x, eig_y, eig_z):
    xb, yb = rhs.shape[1], rhs.shape[2]
    cx, cy = basis_x.shape[1], basis_y.shape[1]
    nb, ci = nx // 2, cx // 2
    ib = ci // nb
    yq = min(yb, 256)
    chunks, mid = yb // yq, ny // 2
    ex = eig_x.reshape(xb // LANES, LANES)
    ey = eig_y.reshape(yb // LANES, LANES)
    ez = eig_z.reshape(1, 1)
    dma = pltpu.SemaphoreType.DMA
    any_space, vmem = pl.BlockSpec(memory_space=pl.ANY), pl.BlockSpec(memory_space=pltpu.VMEM)
    solution, energy = pl.pallas_call(
        functools.partial(kernel, nx, ny, yq),
        name="solve",
        out_shape=(
            jax.ShapeDtypeStruct(rhs.shape, BF16),
            jax.ShapeDtypeStruct((1,), F32),
        ),
        in_specs=[any_space] * 3 + [vmem] * 3,
        out_specs=(any_space, pl.BlockSpec(memory_space=pltpu.SMEM)),
        scratch_shapes=[
            pltpu.VMEM((ny, 2, 2 * xb, ci), BF16),
            pltpu.VMEM((ny, nx, yb, cy), BF16),
            pltpu.VMEM((2 * xb, yb), BF16),
            pltpu.VMEM((ny, nb, 2, ib, yb), BF16),
            pltpu.VMEM((ny, nb - 1, 2, ib, yb), BF16),
            pltpu.VMEM((ny, 2, mid, 2, ib, yb), BF16),
            pltpu.VMEM((nx, 2, 2 * mid * ib, cy), BF16),
            pltpu.VMEM((ny, mid, 2, ib, yb), BF16),
            pltpu.VMEM((chunks, ny, 2, nb * ib, yq), BF16),
            pltpu.VMEM((xb, yb), F32),
            pltpu.VMEM((xb, yb), BF16),
            pltpu.VMEM((nx, xb // LANES, LANES), F32),
            pltpu.VMEM((ny, yb // LANES, LANES), F32),
            pltpu.VMEM((2, 8, LANES), F32),
            pltpu.VMEM((2, 2 * mid * ib, LANES), F32),
            pltpu.VMEM((8, LANES), F32),
            pltpu.VMEM((8, LANES), F32),
            pltpu.VMEM((nx, 8, LANES), F32),
            pltpu.VMEM((2, 8, LANES), F32),
            dma((5,)),
            dma((nx + ny,)), dma((nx + ny,)),
            dma((3,)), dma((3,)),
            dma((ny, 2)), dma((ny,)),
            dma((ny,)), dma((ny,)),
            dma((ny, nx, 2)), dma((ny, nx, 2)),
            dma((ny,)), dma((ny,)),
            dma((ny, 4 * nb - 2)), dma((ny, nx, 2)),
            dma((ny, 2, nb - 1)), dma((ny, 2, nb - 1)),
            dma((ny,)), dma((ny, mid)),
            dma((ny, mid)), dma((ny, mid)),
            dma((chunks, ny)), dma((chunks, ny)),
            dma((chunks, ny)), dma((chunks, 2)),
            dma((chunks, 2, nb - 1)), dma((chunks, 2, nb - 1)),
            dma((chunks,)), dma((chunks,)),
            dma((chunks,)),
            dma((nx + ny,)), dma((nx + ny,)),
        ],
        compiler_params=pltpu.CompilerParams(
            collective_id=0, has_side_effects=True, vmem_limit_bytes=65472 * 1024
        ),
    )(rhs, basis_x, basis_y, ex, ey, ez)
    return solution, energy.reshape(())


def solution(mesh):
    return jax.shard_map(
        functools.partial(shards, mesh.shape["gx"], mesh.shape["gy"]),
        mesh=mesh,
        in_specs=(
            P("gz", "gx", "gy"),
            P("gx", ("gy", "gz")),
            P("gy", ("gx", "gz")),
            P("gx"),
            P("gy"),
            P("gz"),
        ),
        out_specs=(P("gz", "gx", "gy"), P()),
        check_vma=False,
    )
```

```python
import functools

import jax
import jax.numpy as jnp
from jax import lax
from jax.experimental import pallas as pl
from jax.experimental.pallas import tpu as pltpu
from jax.sharding import PartitionSpec as P

BF16, F32 = jnp.bfloat16, jnp.float32
LANES = 128


def contract(left, right, dims):
    return lax.dot_general(left, right, ((dims[:1], dims[1:]), ((), ())), preferred_element_type=F32)


def kernel(
    nx, ny, yq,
    rhs, bx, by, ex, ey, ez,
    out, energy,
    bxb, byb, wide, gs, grecv, gall, wbuf, vrecv, vfull, sown, srecv,
    exall, eyall, ezall, dcol, eacc, e1, e2, e3,
    s_loc, s_eig, r_eig, s_head, r_head, s_bxz, r_bxz, s_bxd, r_bxd, s_byf, r_byf, s_byc, r_byc, s_byp, r_byp,
    s_g, r_g, s_ga, r_ga, s_gd, r_gd, s_vd, r_vd, s_va, r_va, s_vb, r_vb, s_s, r_s, s_out, s_e, r_e,
):
    p, z, c = lax.axis_index("gx"), lax.axis_index("gy"), lax.axis_index("gz")
    px, py = p % 2, p // 2
    nb = nx // 2
    xb, yb = rhs.shape[1], rhs.shape[2]
    cx, cy = bx.shape[1], by.shape[1]
    ci = cx // 2
    ib = ci // nb
    chunks = yb // yq
    half = yb // 2
    other = 1 - c
    mid = ny // 2
    low = z < mid
    works = jnp.logical_or(z == mid - 1, z == mid)
    rests = jnp.logical_not(works)
    place = jnp.where(low, 0, 1)

    def when(condition, act):
        @pl.when(condition)
        def _():
            act()

    def remote(src, dst, ss, rs, **where):
        return pltpu.make_async_remote_copy(
            src_ref=src, dst_ref=dst, send_sem=ss, recv_sem=rs,
            device_id=where, device_id_type=pl.DeviceIdType.MESH,
        )

    def loop(count, body):
        lax.fori_loop(0, count, lambda i, carry: (body(i), carry)[1], 0)

    def cols(start, size):
        return pl.ds(pl.multiple_of(start, LANES), size)

    def rows(start, size):
        return pl.ds(pl.multiple_of(start, size), size)

    barrier = pltpu.get_barrier_semaphore()
    for t in range(1, nx):
        pl.semaphore_signal(barrier, inc=1, device_id={"gx": p ^ t}, device_id_type=pl.DeviceIdType.MESH)
    for d in range(1, ny):
        pl.semaphore_signal(barrier, inc=1, device_id={"gy": (z + d) % ny}, device_id_type=pl.DeviceIdType.MESH)
    pl.semaphore_signal(barrier, inc=1, device_id={"gz": other}, device_id_type=pl.DeviceIdType.MESH)

    mine = rows(px * xb, xb)
    theirs = rows((1 - px) * xb, xb)
    local = [
        pltpu.make_async_copy(by, byb.at[z, p], s_loc.at[0]),
        pltpu.make_async_copy(rhs.at[0], wide.at[mine, :], s_loc.at[1]),
        pltpu.make_async_copy(bx.at[:, cols(px * ci, ci)], bxb.at[z, c, mine, :], s_loc.at[2]),
        pltpu.make_async_copy(ex, exall.at[p], s_loc.at[3]),
        pltpu.make_async_copy(ey, eyall.at[z], s_loc.at[4]),
    ]
    for copy in local:
        copy.start()
    pl.semaphore_wait(barrier, nx + ny - 1)

    swap_bx = remote(bx.at[:, cols((1 - px) * ci, ci)], bxb.at[z, c, mine, :], s_head.at[0], r_head.at[0], gx=p ^ 1)
    swap_bx.start()
    wing = yb // 2

    def swap_rhs(side, part):
        ref = wide.at[side, pl.ds(part * wing, wing)]
        return remote(ref, ref, s_head.at[1 + part], r_head.at[1 + part], gx=p ^ 1)

    eigs = [remote(exall.at[p], exall.at[p], s_eig.at[t], r_eig.at[t], gx=p ^ t) for t in range(1, nx)]
    eigs += [
        remote(eyall.at[z], eyall.at[z], s_eig.at[nx + d], r_eig.at[nx + d], gy=(z + d) % ny) for d in range(1, ny)
    ]
    eigs += [remote(ezall.at[c], ezall.at[c], s_eig.at[0], r_eig.at[0], gz=other)]

    def line(buffer, ss, rs, zs, up, index):
        ref = buffer.at[(zs,) + index]
        return remote(ref, ref, ss.at[zs, 0 if up else 1], rs.at[zs], gy=jnp.clip(z + (1 if up else -1), 0, ny - 1))

    def bx_line(zs, up):
        return line(bxb, s_bxz, r_bxz, zs, up, (c,))

    def by_full(zs, t, part):
        ref = piece(zs, p ^ t, part)
        return remote(
            ref, ref, s_byf.at[zs % mid, t, part], r_byf.at[zs % mid, t, part], gy=jnp.where(low, z + 1, z - 1)
        )

    def by_cross(zs):
        ref = byb.at[zs, p]
        return remote(ref, ref, s_byc.at[zs % mid], r_byc.at[zs % mid], gy=jnp.where(low, mid, mid - 1))

    def across(j):
        return jnp.where(low, mid + j, mid - 1 - j)

    def outside(j):
        return jnp.where(low, z - 1 - j, z + 1 + j)

    def is_outside(j):
        return jnp.where(low, z - 1 - j >= 0, z + 1 + j < ny)

    def goes_on(up):
        return z + 1 < ny if up else z > 0

    def source(r, up):
        zs = z - r if up else z + r
        return zs, jnp.logical_and(zs >= 0, zs < ny)

    def bx_pass(zs):
        return remote(bxb.at[zs, c], bxb.at[zs, c], s_bxd.at[zs], r_bxd.at[zs], gz=other)

    def piece(zs, owner, part):
        return byb.at[zs, owner, pl.ds(part * half, half), :]

    def row_of(zs):
        return jnp.where(zs == z, 0, 1 + zs % mid)

    def plane_direct(zs, t):
        copies = []
        for part in (0, 1) if t == 1 else (1, 0):
            ref = piece(zs, p, part)
            copies.append(remote(ref, ref, s_byp.at[row_of(zs)], r_byp.at[row_of(zs), t - 1, part], gx=p ^ t))
        return copies

    def relay_xy(zs, b):
        ref = piece(zs, p ^ 1, 0)
        return remote(ref, ref, s_byp.at[row_of(zs)], r_byp.at[row_of(zs), 2 * b, 0], gx=p ^ (2 * b))

    def relay_yx(zs, b):
        ref = piece(zs, p ^ (2 * b), 1)
        return remote(ref, ref, s_byp.at[row_of(zs)], r_byp.at[row_of(zs), 2 * b, 1], gx=p ^ 1)

    def wait_piece(zs, t, part):
        ref = piece(zs, p ^ t, part)
        remote(ref, ref, s_byp.at[row_of(zs)], r_byp.at[row_of(zs), t - 1, part], gx=p ^ 1).wait_recv()

    def pass_xy(zs):
        wait_piece(zs, 1, 0)
        for b in range(1, nb):
            relay_xy(zs, b).start()

    def pass_yx(zs):
        for b in range(1, nb):
            wait_piece(zs, 2 * b, 1)
            relay_yx(zs, b).start()

    def plane_y(zs):
        for b in range(1, nb):
            for copy in plane_direct(zs, 2 * b):
                copy.start()

    def plane_x(zs):
        for copy in plane_direct(zs, 1):
            copy.start()

    def g_copies(zs, part):
        lanes = pl.ds(part * wing, wing)
        return [
            remote(
                gs.at[zs, py ^ b, :, :, lanes], grecv.at[zs, b - 1, :, :, lanes],
                s_g.at[zs, part, b - 1], r_g.at[zs, part, b - 1], gx=p ^ (2 * b),
            )
            for b in range(1, nb)
        ]

    def first(zs, part):
        def tile(i):
            cc, n = i // (wing // yq), i % (wing // yq)
            lanes = cols(part * wing + n * yq, yq)
            sums = contract(bxb[zs, cc], wide[:, lanes], (0, 0)).astype(BF16)
            for b in range(nb):
                gs[zs, b, cc, :, lanes] = sums[b * ib : (b + 1) * ib]

        loop(2 * (wing // yq), tile)
        for copy in g_copies(zs, part):
            copy.start()

    def first_whole(zs):
        bx_pass_in(zs).wait_recv()
        first(zs, 0)
        first(zs, 1)

    def first_left(zs):
        bx_pass_in(zs).wait_recv()
        first(zs, 0)

    def first_right(zs):
        first(zs, 1)

    def bx_pass_in(zs):
        return remote(bxb.at[zs, other], bxb.at[zs, other], s_bxd.at[zs], r_bxd.at[zs], gz=other)

    def home(zs):
        return jnp.where(zs < mid, mid - 1, mid)

    def g_send(zs):
        return remote(gs.at[zs, py], gall.at[z, c, zs % mid], s_ga.at[zs], r_ga.at[z, zs % mid], gy=home(zs))

    def g_pass(zs, core, blk):
        ref = gall.at[zs, core, blk]
        return remote(ref, ref, s_gd, r_gd.at[zs, blk], gz=other)

    def collect(zs):
        for part in range(2):
            for copy in g_copies(zs, part):
                copy.wait_recv()

        def tile(i):
            cc, n = i // (yb // yq), i % (yb // yq)
            lanes = cols(n * yq, yq)
            total = gs[zs, py, cc, :, lanes].astype(F32)
            for b in range(1, nb):
                total = total + grecv[zs, b - 1, cc, :, lanes].astype(F32)

            @pl.when(home(zs) != z)
            def _():
                gs[zs, py, cc, :, lanes] = total.astype(BF16)

            @pl.when(home(zs) == z)
            def _():
                gall[z, c, zs % mid, cc, :, lanes] = total.astype(BF16)

        loop(2 * (yb // yq), tile)

        @pl.when(home(zs) != z)
        def _():
            g_send(zs).start()

        @pl.when(home(zs) == z)
        def _():
            g_pass(z, c, zs % mid).start()

    def both(r, act):
        for up in (True, False):
            zs, valid = source(r, up)

            @pl.when(valid)
            def _(zs=zs, up=up):
                act(zs, up)

    def onward(maker, zs, up):
        @pl.when(goes_on(up))
        def _():
            maker(zs, up).start()

    def each(r, act):
        for up in (True, False):
            zs, valid = source(r, up)
            valid = jnp.logical_and(valid, r >= 0 if up else r > 0)

            @pl.when(valid)
            def _(zs=zs):
                act(zs)

    def bx_step(zs, up):
        bx_line(zs, up).wait_recv()
        onward(bx_line, zs, up)
        bx_pass(zs).start()

    def crossing(j):
        zs = across(j)
        by_cross(zs).wait_recv()
        plane_y(zs)
        plane_x(zs)

    def cross_outside(j):
        def act():
            for part in range(2):
                by_full(outside(j), 0, part).wait_recv()
            by_cross(outside(j)).start()

        when(is_outside(j), act)

    def inward(j):
        def act():
            for t in range(nx):
                for part in range(2):
                    by_full(outside(j), t, part).wait_recv()
                    by_full(outside(j), t, part).start()

        when(is_outside(j), act)

    def own_y_inward():
        for b in range(1, nb):
            by_full(z, 2 * b, 1).start()
            wait_piece(z, 2 * b, 0)
            by_full(z, 2 * b, 0).start()

    def own_x_inward():
        wait_piece(z, 1, 1)
        by_full(z, 1, 1).start()

    def own_rest_inward():
        for b in range(1, nb):
            for part in range(2):
                wait_piece(z, 2 * b + 1, part)
                by_full(z, 2 * b + 1, part).start()

    def far_relays(j):
        pass_yx(across(j))
        pass_xy(across(j))

    def round_of(i):
        r = i + 1
        both(r, bx_step)

        @pl.when(r == 1)
        def _():
            when(works, lambda: loop(mid - 1, cross_outside))
            each(1, first_left)
            swap_rhs(theirs, 1).wait_recv()
            first(z, 1)
            each(1, first_right)

        @pl.when(r == 2)
        def _():
            pass_xy(z)
            when(rests, lambda: by_full(z, 1, 0).start())

        @pl.when(r > 1)
        def _():
            each(r, first_whole)

        @pl.when(r == 2)
        def _():
            each(0, collect)
            each(1, collect)
            when(works, lambda: loop(mid - 1, lambda j: crossing(j + 1)))
            if mid > 2:
                when(rests, lambda: loop(mid - 1, inward))

        @pl.when(r == 3)
        def _():
            when(works, lambda: pass_xy(across(0)))

        @pl.when(r > 2)
        def _():
            each(r - 1, collect)

        @pl.when(r == 3)
        def _():
            when(works, lambda: pass_yx(across(0)))
            when(works, lambda: loop(mid - 1, lambda j: far_relays(j + 1)))

        @pl.when(r == 4)
        def _():
            when(rests, own_x_inward)
            when(rests, own_rest_inward)

    local[0].wait()
    when(works, lambda: by_cross(z).start())
    for part in range(2):
        when(rests, lambda part=part: by_full(z, 0, part).start())
    plane_y(z)
    local[1].wait()
    swap_rhs(mine, 0).start()
    swap_rhs(mine, 1).start()
    plane_x(z)
    for copy in local[2:]:
        copy.wait()
    ezall[c] = jnp.broadcast_to(ez[...], (8, LANES))
    for copy in eigs:
        copy.start()
    remote(bx.at[:, cols(px * ci, ci)], bxb.at[z, c, theirs, :], s_head.at[0], r_head.at[0], gx=p ^ 1).wait_recv()
    both(0, lambda zs, up: onward(bx_line, zs, up))
    bx_pass(z).start()

    @pl.when(works)
    def _():
        crossing(0)

    pass_yx(z)
    when(rests, own_y_inward)
    swap_rhs(theirs, 0).wait_recv()
    first_left(z)
    loop(max(ny, 4), round_of)

    for t in range(1, nx):
        remote(exall.at[p ^ t], exall.at[p ^ t], s_eig.at[t], r_eig.at[t], gx=p ^ t).wait_recv()
    for d in range(1, ny):
        far = (z - d) % ny
        remote(eyall.at[far], eyall.at[far], s_eig.at[nx + d], r_eig.at[nx + d], gy=(z + d) % ny).wait_recv()
    remote(ezall.at[other], ezall.at[other], s_eig.at[0], r_eig.at[0], gz=other).wait_recv()
    for blk in range(mid):
        for cc in range(2):
            start = ((place * mid + blk) * 2 + cc) * cx + px * ci + py * ib
            line_at = start // LANES
            per = xb // LANES
            row = exall[line_at // per, pl.ds(line_at % per, 1), :]
            lane = lax.broadcasted_iota(jnp.int32, (ib, LANES), 1)
            want = lax.broadcasted_iota(jnp.int32, (ib, LANES), 0) + start % LANES
            column = jnp.sum(jnp.where(lane == want, jnp.broadcast_to(row, (ib, LANES)), 0.0), axis=1, keepdims=True)
            for k in range(2):
                dcol[k, pl.ds((blk * 2 + cc) * ib, ib), :] = jnp.broadcast_to(column, (ib, LANES)) + ezall[k, 0:1, :]

    def arrive(i):
        zs, blk = (z + 1 + i // mid) % ny, i % mid
        remote(gall.at[zs, c, blk], gall.at[zs, c, blk], s_ga.at[zs], r_ga.at[zs, blk], gy=zs).wait_recv()
        g_pass(zs, c, blk).start()

    def passed(i):
        g_pass(i // mid, other, i % mid).wait_recv()

    @pl.when(works)
    def _():
        loop((ny - 1) * mid, arrive)
        loop(ny * mid, passed)

    eacc[...] = jnp.zeros_like(eacc)

    tn = min(cy, 256)
    ni = 2 * mid * ib

    def second(t):
        owner = p ^ t

        def landed(zs):
            outer = jnp.logical_and((zs < mid) == low, zs != z)

            @pl.when(jnp.logical_and(outer, t > 0))
            def _():
                for part in range(2):
                    by_full(zs, t, part).wait_recv()

            @pl.when(jnp.logical_and(jnp.logical_not(outer), t % 2 == 1))
            def _():
                wait_piece(zs, t, 1)

            @pl.when(jnp.logical_and(jnp.logical_not(outer), t > 1))
            def _():
                wait_piece(zs, t, 0)

        loop(ny, landed)

        def tile(i):
            n, k = i // 2, i % 2
            h = None
            for zs in range(ny):
                term = contract(gall[zs, k].reshape(ni, yb), byb[zs, owner, :, cols(n * tn, tn)], (1, 0))
                h = term if h is None else h + term
            for l in range(tn // LANES):
                line_at = ((owner * 2 + c) * cy + n * tn) // LANES + l
                per = yb // LANES
                row = eyall[line_at // per, pl.ds(line_at % per, 1), :]
                part = h[:, l * LANES : (l + 1) * LANES]
                w = part / (dcol[k] + row)
                eacc[...] += jnp.sum((part * w).reshape(-1, 8, LANES), axis=0)
                wbuf[owner, k, :, cols(n * tn + l * LANES, LANES)] = w.astype(BF16)

        loop(2 * (cy // tn), tile)

    when(works, lambda: loop(nx, second))

    def v_pass(q, zs, core):
        lanes = cols(q * yq, yq)
        return remote(
            gall.at[zs, core, :, :, :, lanes], vrecv.at[zs, :, :, :, lanes], s_vd.at[q], r_vd.at[q, zs], gz=other
        )

    def v_slot(q, side, owner):
        return vfull.at[q, pl.ds(side * mid, mid), :, pl.ds(pl.multiple_of(owner * ib, ib), ib), :]

    def v_send(q, zs):
        return remote(
            gall.at[zs, c, :, :, :, cols(q * yq, yq)], v_slot(q, place, py), s_va.at[q], r_va.at[q, place], gy=zs
        )

    def v_copies(q, side):
        slot = v_slot(q, side, py)
        return [
            remote(slot, slot, s_vb.at[q, side, b - 1], r_vb.at[q, side, b - 1], gx=p ^ (2 * b)) for b in range(1, nb)
        ]

    def target_of(d):
        end = jnp.where(d % 2 == 0, ny - 1 - d // 2, d // 2)
        return jnp.where(low, end, ny - 1 - end)

    def third(q, d):
        zs = target_of(d)

        def mode(i):
            k = jnp.where(i == 0, other, c)
            v = None
            for owner in range(nx):
                term = contract(wbuf[owner, k], byb[zs, owner, rows(q * yq, yq), :], (1, 1))
                v = term if v is None else v + term
            gall[zs, k, :, :, :, cols(q * yq, yq)] = v.astype(BF16).reshape(mid, 2, ib, yq)
            when(i == 0, lambda: v_pass(q, zs, other).start())

        loop(2, mode)

    def merge(q, d):
        zs = target_of(d)
        lanes = cols(q * yq, yq)
        v_pass(q, zs, c).wait_recv()
        v = (gall[zs, c, :, :, :, lanes].astype(F32) + vrecv[zs, :, :, :, lanes].astype(F32)).astype(BF16)

        @pl.when(zs != z)
        def _():
            gall[zs, c, :, :, :, lanes] = v
            v_send(q, zs).start()

        @pl.when(zs == z)
        def _():
            vfull[q, pl.ds(place * mid, mid), :, pl.ds(pl.multiple_of(py * ib, ib), ib), :] = v
            for copy in v_copies(q, place):
                copy.start()

    def spread(q):
        def target(i):
            side = jnp.where(low, i, 1 - i)

            @pl.when(mid - 1 + side != z)
            def _():
                slot = v_slot(q, side, py)
                remote(slot, slot, s_va.at[q], r_va.at[q, side], gy=(z + 1) % ny).wait_recv()
                for copy in v_copies(q, side):
                    copy.start()

        loop(2, target)

    mt = min(xb, 512)

    def s_copy(q, m):
        lanes = cols(q * yq, yq)
        return remote(
            wide.at[rows((1 - px) * xb + m * mt, mt), lanes], srecv.at[rows(m * mt, mt), lanes],
            s_s.at[q, m], r_s.at[q, m], gx=p ^ 1,
        )

    def fourth(q):
        lanes = cols(q * yq, yq)

        def landed(side):
            for b in range(1, nb):
                slot = v_slot(q, side, py ^ b)
                remote(slot, slot, s_vb.at[q, side, b - 1], r_vb.at[q, side, b - 1], gx=p ^ (2 * b)).wait_recv()

        loop(2, landed)

        def tile(i):
            m, own = i % (xb // mt), i // (xb // mt)
            side = jnp.where(own == 1, px, 1 - px)
            at = rows(side * xb + m * mt, mt)
            s = None
            for zs in range(ny):
                for cc in range(2):
                    term = contract(bxb[zs, cc, at, :], vfull[q, zs, cc], (1, 0))
                    s = term if s is None else s + term

            @pl.when(own == 0)
            def _():
                wide[at, lanes] = s.astype(BF16)
                s_copy(q, m).start()

            @pl.when(own == 1)
            def _():
                sown[rows(m * mt, mt), lanes] = s

        loop(2 * (xb // mt), tile)

    def out_copy(q, m):
        lanes = cols(q * yq, yq)
        return pltpu.make_async_copy(
            wide.at[rows(px * xb + m * mt, mt), lanes], out.at[0, rows(m * mt, mt), lanes], s_out.at[q, m]
        )

    def finish(q):
        lanes = cols(q * yq, yq)

        def tile(m):
            at = rows(m * mt, mt)
            s_copy(q, m).wait_recv()
            wide[rows(px * xb + m * mt, mt), lanes] = (sown[at, lanes] + srecv[at, lanes].astype(F32)).astype(BF16)
            out_copy(q, m).start()

        loop(xb // mt, tile)

    @pl.when(works)
    def _():
        remote(gall.at[:, c], gall.at[:, c], s_gd, r_gd.at[0, 0], gz=other).wait_send()

    swap_rhs(mine, 0).wait_send()
    swap_rhs(mine, 1).wait_send()

    e_core = remote(eacc, e1, s_e.at[0], r_e.at[0], gz=other)
    e_plane = [remote(e2.at[p], e2.at[p], s_e.at[t], r_e.at[t], gx=p ^ t) for t in range(1, nx)]
    e_line = [remote(e3.at[place], e3.at[place], s_e.at[nx + d], r_e.at[nx + place], gy=(z + d) % ny) for d in range(1, ny)]

    def leave(q):
        def step(d):
            start = q == 0

            @pl.when(jnp.logical_and(start, d == 0))
            def _():
                e_core.start()

            @pl.when(jnp.logical_and(start, d == 2))
            def _():
                e_core.wait_recv()
                e2[p] = eacc[...] + e1[...]
                for copy in e_plane:
                    copy.start()

            @pl.when(jnp.logical_and(start, d == ny + 1))
            def _():
                for s in range(1, nx):
                    remote(e2.at[p ^ s], e2.at[p ^ s], s_e.at[s], r_e.at[s], gx=p ^ s).wait_recv()
                total = e2[0]
                for s in range(1, nx):
                    total = total + e2[s]
                e3[place] = total
                for copy in e_line:
                    copy.start()

            @pl.when(d < ny)
            def _():
                third(q, d)

            @pl.when(jnp.logical_and(start, d >= 2))
            def _():
                merge(q, d - 2)

        loop(ny + 2, step)

    def stage(t, lag, act):
        @pl.when(jnp.logical_and(t >= lag, t < chunks + lag))
        def _():
            act(t - lag)

    def tail(t):
        stage(t, 0, lambda q: when(works, lambda: leave(q)))
        stage(t, 1, spread)

        @pl.when(jnp.logical_and(works, jnp.logical_and(t >= 1, t < chunks)))
        def _():
            loop(ny, lambda d: merge(t, d))

        stage(t, 2, fourth)
        stage(t, 3, finish)

    loop(chunks + 3, tail)

    for side in range(2):
        @pl.when(mid - 1 + side != z)
        def _(side=side):
            remote(e3.at[side], e3.at[side], s_e.at[0], r_e.at[nx + side], gy=(z + 1) % ny).wait_recv()

    total = e3[0] + e3[1]
    energy[0] = jnp.sum(total)

    swap_bx.wait_send()
    for copy in eigs:
        copy.wait_send()

    @pl.when(works)
    def _():
        for copy in [e_core] + e_plane + e_line:
            copy.wait_send()

    def plane_drain(zs):
        sent = byb.at[zs, pl.ds(0, 2 * nb - 1)]
        remote(sent, sent, s_byp.at[row_of(zs)], r_byp.at[0, 0, 0], gx=p ^ 1).wait_send()

    def drain(zs):
        for up in (True, False):
            from_here = zs <= z if up else zs >= z

            @pl.when(jnp.logical_and(goes_on(up), from_here))
            def _(up=up):
                bx_line(zs, up).wait_send()

        bx_pass(zs).wait_send()
        for part in range(2):
            for copy in g_copies(zs, part):
                copy.wait_send()
        same = (zs < mid) == low
        when(jnp.logical_or(zs == z, jnp.logical_and(works, jnp.logical_not(same))), lambda: plane_drain(zs))
        when(jnp.logical_and(works, same), lambda: by_cross(zs).wait_send())

        @pl.when(jnp.logical_and(jnp.logical_and(jnp.logical_not(works), same), jnp.where(low, zs <= z, zs >= z)))
        def _():
            for t in range(nx):
                for part in range(2):
                    by_full(zs, t, part).wait_send()

        when(home(zs) != z, lambda: g_send(zs).wait_send())

    loop(ny, drain)

    def drain_chunk(q):
        @pl.when(works)
        def _():
            lanes = cols(q * yq, yq)
            passed_on, sent = vrecv.at[:, :, :, :, lanes], vrecv.at[pl.ds(0, ny - 1), :, :, :, lanes]
            remote(passed_on, passed_on, s_vd.at[q], r_vd.at[q, 0], gz=other).wait_send()
            remote(sent, sent, s_va.at[q], r_va.at[q, 0], gy=(z + 1) % ny).wait_send()

        for side in range(2):
            for copy in v_copies(q, side):
                copy.wait_send()

        def tile(m):
            s_copy(q, m).wait_send()
            out_copy(q, m).wait()

        loop(xb // mt, tile)

    loop(chunks, drain_chunk)


def shards(nx, ny, rhs, basis_x, basis_y, eig_x, eig_y, eig_z):
    xb, yb = rhs.shape[1], rhs.shape[2]
    cx, cy = basis_x.shape[1], basis_y.shape[1]
    nb, ci = nx // 2, cx // 2
    ib = ci // nb
    yq = min(yb, 256)
    chunks, mid, tiles = yb // yq, ny // 2, xb // min(xb, 512)
    ex = eig_x.reshape(xb // LANES, LANES)
    ey = eig_y.reshape(yb // LANES, LANES)
    ez = eig_z.reshape(1, 1)
    dma = pltpu.SemaphoreType.DMA
    any_space, vmem = pl.BlockSpec(memory_space=pl.ANY), pl.BlockSpec(memory_space=pltpu.VMEM)
    solution, energy = pl.pallas_call(
        functools.partial(kernel, nx, ny, yq),
        name="solve",
        out_shape=(
            jax.ShapeDtypeStruct(rhs.shape, BF16),
            jax.ShapeDtypeStruct((1,), F32),
        ),
        in_specs=[any_space] * 3 + [vmem] * 3,
        out_specs=(any_space, pl.BlockSpec(memory_space=pltpu.SMEM)),
        scratch_shapes=[
            pltpu.VMEM((ny, 2, 2 * xb, ci), BF16),
            pltpu.VMEM((ny, nx, yb, cy), BF16),
            pltpu.VMEM((2 * xb, yb), BF16),
            pltpu.VMEM((ny, nb, 2, ib, yb), BF16),
            pltpu.VMEM((ny, nb - 1, 2, ib, yb), BF16),
            pltpu.VMEM((ny, 2, mid, 2, ib, yb), BF16),
            pltpu.VMEM((nx, 2, 2 * mid * ib, cy), BF16),
            pltpu.VMEM((ny, mid, 2, ib, yb), BF16),
            pltpu.VMEM((chunks, ny, 2, nb * ib, yq), BF16),
            pltpu.VMEM((xb, yb), F32),
            pltpu.VMEM((xb, yb), BF16),
            pltpu.VMEM((nx, xb // LANES, LANES), F32),
            pltpu.VMEM((ny, yb // LANES, LANES), F32),
            pltpu.VMEM((2, 8, LANES), F32),
            pltpu.VMEM((2, 2 * mid * ib, LANES), F32),
            pltpu.VMEM((8, LANES), F32),
            pltpu.VMEM((8, LANES), F32),
            pltpu.VMEM((nx, 8, LANES), F32),
            pltpu.VMEM((2, 8, LANES), F32),
            dma((5,)),
            dma((nx + ny,)), dma((nx + ny,)),
            dma((3,)), dma((3,)),
            dma((ny, 2)), dma((ny,)),
            dma((ny,)), dma((ny,)),
            dma((mid, nx, 2)), dma((mid, nx, 2)),
            dma((mid,)), dma((mid,)),
            dma((mid + 1,)), dma((mid + 1, nx - 1, 2)),
            dma((ny, 2, nb - 1)), dma((ny, 2, nb - 1)),
            dma((ny,)), dma((ny, mid)),
            pltpu.SemaphoreType.DMA, dma((ny, mid)),
            dma((chunks,)), dma((chunks, ny)),
            dma((chunks,)), dma((chunks, 2)),
            dma((chunks, 2, nb - 1)), dma((chunks, 2, nb - 1)),
            dma((chunks, tiles)), dma((chunks, tiles)),
            dma((chunks, tiles)),
            dma((nx + ny,)), dma((nx + ny,)),
        ],
        compiler_params=pltpu.CompilerParams(
            collective_id=0, has_side_effects=True, vmem_limit_bytes=65472 * 1024
        ),
    )(rhs, basis_x, basis_y, ex, ey, ez)
    return solution, energy.reshape(())


def solution(mesh):
    return jax.shard_map(
        functools.partial(shards, mesh.shape["gx"], mesh.shape["gy"]),
        mesh=mesh,
        in_specs=(
            P("gz", "gx", "gy"),
            P("gx", ("gy", "gz")),
            P("gy", ("gx", "gz")),
            P("gx"),
            P("gy"),
            P("gz"),
        ),
        out_specs=(P("gz", "gx", "gy"), P()),
        check_vma=False,
    )
```

```python
import functools

import jax
import jax.numpy as jnp
from jax import lax
from jax.experimental import pallas as pl
from jax.experimental.pallas import tpu as pltpu
from jax.sharding import PartitionSpec as P

BF16, F32 = jnp.bfloat16, jnp.float32
LANES = 128


def contract(left, right, dims):
    return lax.dot_general(left, right, ((dims[:1], dims[1:]), ((), ())), preferred_element_type=F32)


def kernel(
    nx, ny, yq,
    rhs, bx, by, ex, ey, ez,
    out, energy,
    bxb, byb, wide, gs, grecv, gall, wbuf, vrecv, vfull, sown, srecv,
    exall, eyall, ezall, dcol, eacc, e1, e2, e3,
    s_loc, s_eig, r_eig, s_head, r_head, s_bxz, r_bxz, s_bxd, r_bxd, s_byf, r_byf, s_byc, r_byc, s_byp, r_byp,
    s_g, r_g, s_ga, r_ga, s_gd, r_gd, s_vd, r_vd, s_va, r_va, s_vb, r_vb, s_s, r_s, s_out, s_e, r_e,
):
    p, z, c = lax.axis_index("gx"), lax.axis_index("gy"), lax.axis_index("gz")
    px, py = p % 2, p // 2
    nb = nx // 2
    xb, yb = rhs.shape[1], rhs.shape[2]
    cx, cy = bx.shape[1], by.shape[1]
    ci = cx // 2
    ib = ci // nb
    chunks = yb // yq
    half = yb // 2
    other = 1 - c
    mid = ny // 2
    low = z < mid
    works = jnp.logical_or(z == mid - 1, z == mid)
    rests = jnp.logical_not(works)
    place = jnp.where(low, 0, 1)

    def when(condition, act):
        @pl.when(condition)
        def _():
            act()

    def remote(src, dst, ss, rs, **where):
        return pltpu.make_async_remote_copy(
            src_ref=src, dst_ref=dst, send_sem=ss, recv_sem=rs,
            device_id=where, device_id_type=pl.DeviceIdType.MESH,
        )

    def loop(count, body):
        lax.fori_loop(0, count, lambda i, carry: (body(i), carry)[1], 0)

    def cols(start, size):
        return pl.ds(pl.multiple_of(start, LANES), size)

    def rows(start, size):
        return pl.ds(pl.multiple_of(start, size), size)

    barrier = pltpu.get_barrier_semaphore()
    for t in range(1, nx):
        pl.semaphore_signal(barrier, inc=1, device_id={"gx": p ^ t}, device_id_type=pl.DeviceIdType.MESH)
    for d in range(1, ny):
        pl.semaphore_signal(barrier, inc=1, device_id={"gy": (z + d) % ny}, device_id_type=pl.DeviceIdType.MESH)
    pl.semaphore_signal(barrier, inc=1, device_id={"gz": other}, device_id_type=pl.DeviceIdType.MESH)

    mine = rows(px * xb, xb)
    theirs = rows((1 - px) * xb, xb)
    local = [
        pltpu.make_async_copy(by, byb.at[z, p], s_loc.at[0]),
        pltpu.make_async_copy(rhs.at[0], wide.at[mine, :], s_loc.at[1]),
        pltpu.make_async_copy(bx.at[:, cols(px * ci, ci)], bxb.at[z, c, mine, :], s_loc.at[2]),
        pltpu.make_async_copy(ex, exall.at[p], s_loc.at[3]),
        pltpu.make_async_copy(ey, eyall.at[z], s_loc.at[4]),
    ]
    for copy in local:
        copy.start()
    pl.semaphore_wait(barrier, nx + ny - 1)

    swap_bx = remote(bx.at[:, cols((1 - px) * ci, ci)], bxb.at[z, c, mine, :], s_head.at[0], r_head.at[0], gx=p ^ 1)
    swap_bx.start()
    wing = yb // 2

    def swap_rhs(side, part):
        ref = wide.at[side, pl.ds(part * wing, wing)]
        return remote(ref, ref, s_head.at[1 + part], r_head.at[1 + part], gx=p ^ 1)

    eigs = [remote(exall.at[p], exall.at[p], s_eig.at[t], r_eig.at[t], gx=p ^ t) for t in range(1, nx)]
    eigs += [
        remote(eyall.at[z], eyall.at[z], s_eig.at[nx + d], r_eig.at[nx + d], gy=(z + d) % ny) for d in range(1, ny)
    ]
    eigs += [remote(ezall.at[c], ezall.at[c], s_eig.at[0], r_eig.at[0], gz=other)]

    def line(buffer, ss, rs, zs, up, index):
        ref = buffer.at[(zs,) + index]
        return remote(ref, ref, ss.at[zs, 0 if up else 1], rs.at[zs], gy=jnp.clip(z + (1 if up else -1), 0, ny - 1))

    def bx_line(zs, up):
        return line(bxb, s_bxz, r_bxz, zs, up, (c,))

    def by_full(zs, t, part):
        ref = piece(zs, p ^ t, part)
        return remote(
            ref, ref, s_byf.at[zs % mid, t, part], r_byf.at[zs % mid, t, part], gy=jnp.where(low, z + 1, z - 1)
        )

    def by_cross(zs):
        ref = byb.at[zs, p]
        return remote(ref, ref, s_byc.at[zs % mid], r_byc.at[zs % mid], gy=jnp.where(low, mid, mid - 1))

    def across(j):
        return jnp.where(low, mid + j, mid - 1 - j)

    def outside(j):
        return jnp.where(low, z - 1 - j, z + 1 + j)

    def is_outside(j):
        return jnp.where(low, z - 1 - j >= 0, z + 1 + j < ny)

    def goes_on(up):
        return z + 1 < ny if up else z > 0

    def source(r, up):
        zs = z - r if up else z + r
        return zs, jnp.logical_and(zs >= 0, zs < ny)

    def bx_pass(zs):
        return remote(bxb.at[zs, c], bxb.at[zs, c], s_bxd.at[zs], r_bxd.at[zs], gz=other)

    def piece(zs, owner, part):
        return byb.at[zs, owner, pl.ds(part * half, half), :]

    def row_of(zs):
        return jnp.where(zs == z, 0, 1 + zs % mid)

    def plane_direct(zs, t):
        copies = []
        for part in (0, 1) if t == 1 else (1, 0):
            ref = piece(zs, p, part)
            copies.append(remote(ref, ref, s_byp.at[row_of(zs)], r_byp.at[row_of(zs), t - 1, part], gx=p ^ t))
        return copies

    def relay_xy(zs, b):
        ref = piece(zs, p ^ 1, 0)
        return remote(ref, ref, s_byp.at[row_of(zs)], r_byp.at[row_of(zs), 2 * b, 0], gx=p ^ (2 * b))

    def relay_yx(zs, b):
        ref = piece(zs, p ^ (2 * b), 1)
        return remote(ref, ref, s_byp.at[row_of(zs)], r_byp.at[row_of(zs), 2 * b, 1], gx=p ^ 1)

    def wait_piece(zs, t, part):
        ref = piece(zs, p ^ t, part)
        remote(ref, ref, s_byp.at[row_of(zs)], r_byp.at[row_of(zs), t - 1, part], gx=p ^ 1).wait_recv()

    def pass_xy(zs):
        wait_piece(zs, 1, 0)
        for b in range(1, nb):
            relay_xy(zs, b).start()

    def pass_yx(zs):
        for b in range(1, nb):
            wait_piece(zs, 2 * b, 1)
            relay_yx(zs, b).start()

    def plane_y(zs):
        for b in range(1, nb):
            for copy in plane_direct(zs, 2 * b):
                copy.start()

    def plane_x(zs):
        for copy in plane_direct(zs, 1):
            copy.start()

    def g_copies(zs, part):
        lanes = pl.ds(part * wing, wing)
        return [
            remote(
                gs.at[zs, py ^ b, :, :, lanes], grecv.at[zs, b - 1, :, :, lanes],
                s_g.at[zs, part, b - 1], r_g.at[zs, part, b - 1], gx=p ^ (2 * b),
            )
            for b in range(1, nb)
        ]

    def first(zs, part):
        def tile(i):
            cc, n = i // (wing // yq), i % (wing // yq)
            lanes = cols(part * wing + n * yq, yq)
            sums = contract(bxb[zs, cc], wide[:, lanes], (0, 0)).astype(BF16)
            for b in range(nb):
                gs[zs, b, cc, :, lanes] = sums[b * ib : (b + 1) * ib]

        loop(2 * (wing // yq), tile)
        for copy in g_copies(zs, part):
            copy.start()

    def first_whole(zs):
        bx_pass_in(zs).wait_recv()
        first(zs, 0)
        first(zs, 1)

    def first_left(zs):
        bx_pass_in(zs).wait_recv()
        first(zs, 0)

    def first_right(zs):
        first(zs, 1)

    def bx_pass_in(zs):
        return remote(bxb.at[zs, other], bxb.at[zs, other], s_bxd.at[zs], r_bxd.at[zs], gz=other)

    def home(zs):
        return jnp.where(zs < mid, mid - 1, mid)

    def g_send(zs):
        return remote(gs.at[zs, py], gall.at[z, c, zs % mid], s_ga.at[zs], r_ga.at[z, zs % mid], gy=home(zs))

    def g_pass(zs, core, blk):
        ref = gall.at[zs, core, blk]
        return remote(ref, ref, s_gd, r_gd.at[zs, blk], gz=other)

    def collect(zs):
        for part in range(2):
            for copy in g_copies(zs, part):
                copy.wait_recv()

        def tile(i):
            cc, n = i // (yb // yq), i % (yb // yq)
            lanes = cols(n * yq, yq)
            total = gs[zs, py, cc, :, lanes].astype(F32)
            for b in range(1, nb):
                total = total + grecv[zs, b - 1, cc, :, lanes].astype(F32)

            @pl.when(home(zs) != z)
            def _():
                gs[zs, py, cc, :, lanes] = total.astype(BF16)

            @pl.when(home(zs) == z)
            def _():
                gall[z, c, zs % mid, cc, :, lanes] = total.astype(BF16)

        loop(2 * (yb // yq), tile)

        @pl.when(home(zs) != z)
        def _():
            g_send(zs).start()

        @pl.when(home(zs) == z)
        def _():
            g_pass(z, c, zs % mid).start()

    def both(r, act):
        for up in (True, False):
            zs, valid = source(r, up)

            @pl.when(valid)
            def _(zs=zs, up=up):
                act(zs, up)

    def onward(maker, zs, up):
        @pl.when(goes_on(up))
        def _():
            maker(zs, up).start()

    def each(r, act):
        for up in (True, False):
            zs, valid = source(r, up)
            valid = jnp.logical_and(valid, r >= 0 if up else r > 0)

            @pl.when(valid)
            def _(zs=zs):
                act(zs)

    def bx_step(zs, up):
        bx_line(zs, up).wait_recv()
        onward(bx_line, zs, up)
        bx_pass(zs).start()

    def crossing(j):
        zs = across(j)
        by_cross(zs).wait_recv()
        plane_y(zs)
        plane_x(zs)

    def cross_outside(j):
        def act():
            for part in range(2):
                by_full(outside(j), 0, part).wait_recv()
            by_cross(outside(j)).start()

        when(is_outside(j), act)

    def inward_first(j):
        def act():
            for part in range(2):
                by_full(outside(j), 0, part).wait_recv()
                by_full(outside(j), 0, part).start()

        when(is_outside(j), act)

    def inward(j):
        def act():
            for t in range(1, nx):
                for part in range(2):
                    by_full(outside(j), t, part).wait_recv()
                    by_full(outside(j), t, part).start()

        when(is_outside(j), act)

    def own_y_inward():
        for b in range(1, nb):
            by_full(z, 2 * b, 1).start()
            wait_piece(z, 2 * b, 0)
            by_full(z, 2 * b, 0).start()

    def own_x_inward():
        wait_piece(z, 1, 1)
        by_full(z, 1, 1).start()

    def own_rest_inward():
        for b in range(1, nb):
            for part in range(2):
                wait_piece(z, 2 * b + 1, part)
                by_full(z, 2 * b + 1, part).start()

    def far_relays(j):
        pass_yx(across(j))
        pass_xy(across(j))

    def round_of(i):
        r = i + 1
        both(r, bx_step)

        @pl.when(r == 1)
        def _():
            when(works, lambda: loop(mid - 1, cross_outside))
            if mid > 2:
                when(rests, lambda: loop(mid - 1, inward_first))
            each(1, first_left)
            swap_rhs(theirs, 1).wait_recv()
            first(z, 1)
            each(1, first_right)

        @pl.when(r == 2)
        def _():
            pass_xy(z)
            when(rests, lambda: by_full(z, 1, 0).start())

        @pl.when(r > 1)
        def _():
            each(r, first_whole)

        @pl.when(r == 2)
        def _():
            each(0, collect)
            each(1, collect)
            when(works, lambda: loop(mid - 1, lambda j: crossing(j + 1)))

        @pl.when(r == 3)
        def _():
            when(works, lambda: pass_xy(across(0)))

        @pl.when(r > 2)
        def _():
            each(r - 1, collect)

        @pl.when(r == 3)
        def _():
            when(works, lambda: pass_yx(across(0)))
            when(works, lambda: loop(mid - 1, lambda j: far_relays(j + 1)))

        @pl.when(r == 4)
        def _():
            when(rests, own_x_inward)
            when(rests, own_rest_inward)

    local[0].wait()
    when(works, lambda: by_cross(z).start())
    for part in range(2):
        when(rests, lambda part=part: by_full(z, 0, part).start())
    plane_y(z)
    local[1].wait()
    swap_rhs(mine, 0).start()
    swap_rhs(mine, 1).start()
    plane_x(z)
    for copy in local[2:]:
        copy.wait()
    ezall[c] = jnp.broadcast_to(ez[...], (8, LANES))
    for copy in eigs:
        copy.start()
    remote(bx.at[:, cols(px * ci, ci)], bxb.at[z, c, theirs, :], s_head.at[0], r_head.at[0], gx=p ^ 1).wait_recv()
    both(0, lambda zs, up: onward(bx_line, zs, up))
    bx_pass(z).start()

    @pl.when(works)
    def _():
        crossing(0)

    pass_yx(z)
    when(rests, own_y_inward)
    swap_rhs(theirs, 0).wait_recv()
    first_left(z)
    loop(max(ny, 4), round_of)
    if mid > 2:
        when(rests, lambda: loop(mid - 1, inward))

    for t in range(1, nx):
        remote(exall.at[p ^ t], exall.at[p ^ t], s_eig.at[t], r_eig.at[t], gx=p ^ t).wait_recv()
    for d in range(1, ny):
        far = (z - d) % ny
        remote(eyall.at[far], eyall.at[far], s_eig.at[nx + d], r_eig.at[nx + d], gy=(z + d) % ny).wait_recv()
    remote(ezall.at[other], ezall.at[other], s_eig.at[0], r_eig.at[0], gz=other).wait_recv()
    for blk in range(mid):
        for cc in range(2):
            start = ((place * mid + blk) * 2 + cc) * cx + px * ci + py * ib
            line_at = start // LANES
            per = xb // LANES
            row = exall[line_at // per, pl.ds(line_at % per, 1), :]
            lane = lax.broadcasted_iota(jnp.int32, (ib, LANES), 1)
            want = lax.broadcasted_iota(jnp.int32, (ib, LANES), 0) + start % LANES
            column = jnp.sum(jnp.where(lane == want, jnp.broadcast_to(row, (ib, LANES)), 0.0), axis=1, keepdims=True)
            for k in range(2):
                dcol[k, pl.ds((blk * 2 + cc) * ib, ib), :] = jnp.broadcast_to(column, (ib, LANES)) + ezall[k, 0:1, :]

    def arrive(i):
        zs, blk = (z + 1 + i // mid) % ny, i % mid
        remote(gall.at[zs, c, blk], gall.at[zs, c, blk], s_ga.at[zs], r_ga.at[zs, blk], gy=zs).wait_recv()
        g_pass(zs, c, blk).start()

    def passed(i):
        g_pass(i // mid, other, i % mid).wait_recv()

    @pl.when(works)
    def _():
        loop((ny - 1) * mid, arrive)
        loop(ny * mid, passed)

    eacc[...] = jnp.zeros_like(eacc)

    tn = min(cy, 256)
    ni = 2 * mid * ib

    def second(t):
        owner = p ^ t

        def landed(zs):
            outer = jnp.logical_and((zs < mid) == low, zs != z)

            @pl.when(jnp.logical_and(outer, t > 0))
            def _():
                for part in range(2):
                    by_full(zs, t, part).wait_recv()

            @pl.when(jnp.logical_and(jnp.logical_not(outer), t % 2 == 1))
            def _():
                wait_piece(zs, t, 1)

            @pl.when(jnp.logical_and(jnp.logical_not(outer), t > 1))
            def _():
                wait_piece(zs, t, 0)

        loop(ny, landed)

        def tile(i):
            n, k = i // 2, i % 2
            h = None
            for zs in range(ny):
                term = contract(gall[zs, k].reshape(ni, yb), byb[zs, owner, :, cols(n * tn, tn)], (1, 0))
                h = term if h is None else h + term
            for l in range(tn // LANES):
                line_at = ((owner * 2 + c) * cy + n * tn) // LANES + l
                per = yb // LANES
                row = eyall[line_at // per, pl.ds(line_at % per, 1), :]
                part = h[:, l * LANES : (l + 1) * LANES]
                w = part / (dcol[k] + row)
                eacc[...] += jnp.sum((part * w).reshape(-1, 8, LANES), axis=0)
                wbuf[owner, k, :, cols(n * tn + l * LANES, LANES)] = w.astype(BF16)

        loop(2 * (cy // tn), tile)

    when(works, lambda: loop(nx, second))

    def v_pass(q, zs, core):
        lanes = cols(q * yq, yq)
        return remote(
            gall.at[zs, core, :, :, :, lanes], vrecv.at[zs, :, :, :, lanes], s_vd.at[q], r_vd.at[q, zs], gz=other
        )

    def v_slot(q, side, owner):
        return vfull.at[q, pl.ds(side * mid, mid), :, pl.ds(pl.multiple_of(owner * ib, ib), ib), :]

    def v_send(q, zs):
        return remote(
            gall.at[zs, c, :, :, :, cols(q * yq, yq)], v_slot(q, place, py), s_va.at[q], r_va.at[q, place], gy=zs
        )

    def v_copies(q, side):
        slot = v_slot(q, side, py)
        return [
            remote(slot, slot, s_vb.at[q, side, b - 1], r_vb.at[q, side, b - 1], gx=p ^ (2 * b)) for b in range(1, nb)
        ]

    def target_of(d):
        end = jnp.where(d % 2 == 0, ny - 1 - d // 2, d // 2)
        return jnp.where(low, end, ny - 1 - end)

    def third(q, d):
        zs = target_of(d)

        def mode(i):
            k = jnp.where(i == 0, other, c)
            v = None
            for owner in range(nx):
                term = contract(wbuf[owner, k], byb[zs, owner, rows(q * yq, yq), :], (1, 1))
                v = term if v is None else v + term
            gall[zs, k, :, :, :, cols(q * yq, yq)] = v.astype(BF16).reshape(mid, 2, ib, yq)
            when(i == 0, lambda: v_pass(q, zs, other).start())

        loop(2, mode)

    def merge(q, d):
        zs = target_of(d)
        lanes = cols(q * yq, yq)
        v_pass(q, zs, c).wait_recv()
        v = (gall[zs, c, :, :, :, lanes].astype(F32) + vrecv[zs, :, :, :, lanes].astype(F32)).astype(BF16)

        @pl.when(zs != z)
        def _():
            gall[zs, c, :, :, :, lanes] = v
            v_send(q, zs).start()

        @pl.when(zs == z)
        def _():
            vfull[q, pl.ds(place * mid, mid), :, pl.ds(pl.multiple_of(py * ib, ib), ib), :] = v
            for copy in v_copies(q, place):
                copy.start()

    def spread(q):
        def target(i):
            side = jnp.where(low, i, 1 - i)

            @pl.when(mid - 1 + side != z)
            def _():
                slot = v_slot(q, side, py)
                remote(slot, slot, s_va.at[q], r_va.at[q, side], gy=(z + 1) % ny).wait_recv()
                for copy in v_copies(q, side):
                    copy.start()

        loop(2, target)

    mt = min(xb, 512)

    def s_copy(q, m):
        lanes = cols(q * yq, yq)
        return remote(
            wide.at[rows((1 - px) * xb + m * mt, mt), lanes], srecv.at[rows(m * mt, mt), lanes],
            s_s.at[q, m], r_s.at[q, m], gx=p ^ 1,
        )

    def fourth(q):
        lanes = cols(q * yq, yq)

        def landed(side):
            for b in range(1, nb):
                slot = v_slot(q, side, py ^ b)
                remote(slot, slot, s_vb.at[q, side, b - 1], r_vb.at[q, side, b - 1], gx=p ^ (2 * b)).wait_recv()

        loop(2, landed)

        def tile(i):
            m, own = i % (xb // mt), i // (xb // mt)
            side = jnp.where(own == 1, px, 1 - px)
            at = rows(side * xb + m * mt, mt)
            s = None
            for zs in range(ny):
                for cc in range(2):
                    term = contract(bxb[zs, cc, at, :], vfull[q, zs, cc], (1, 0))
                    s = term if s is None else s + term

            @pl.when(own == 0)
            def _():
                wide[at, lanes] = s.astype(BF16)
                s_copy(q, m).start()

            @pl.when(own == 1)
            def _():
                sown[rows(m * mt, mt), lanes] = s

        loop(2 * (xb // mt), tile)

    def out_copy(q, m):
        lanes = cols(q * yq, yq)
        return pltpu.make_async_copy(
            wide.at[rows(px * xb + m * mt, mt), lanes], out.at[0, rows(m * mt, mt), lanes], s_out.at[q, m]
        )

    def finish(q):
        lanes = cols(q * yq, yq)

        def tile(m):
            at = rows(m * mt, mt)
            s_copy(q, m).wait_recv()
            wide[rows(px * xb + m * mt, mt), lanes] = (sown[at, lanes] + srecv[at, lanes].astype(F32)).astype(BF16)
            out_copy(q, m).start()

        loop(xb // mt, tile)

    @pl.when(works)
    def _():
        remote(gall.at[:, c], gall.at[:, c], s_gd, r_gd.at[0, 0], gz=other).wait_send()

    swap_rhs(mine, 0).wait_send()
    swap_rhs(mine, 1).wait_send()

    e_core = remote(eacc, e1, s_e.at[0], r_e.at[0], gz=other)
    e_plane = [remote(e2.at[p], e2.at[p], s_e.at[t], r_e.at[t], gx=p ^ t) for t in range(1, nx)]
    e_line = [remote(e3.at[place], e3.at[place], s_e.at[nx + d], r_e.at[nx + place], gy=(z + d) % ny) for d in range(1, ny)]

    def leave(q):
        def step(d):
            start = q == 0

            @pl.when(jnp.logical_and(start, d == 0))
            def _():
                e_core.start()

            @pl.when(jnp.logical_and(start, d == 2))
            def _():
                e_core.wait_recv()
                e2[p] = eacc[...] + e1[...]
                for copy in e_plane:
                    copy.start()

            @pl.when(jnp.logical_and(start, d == ny + 1))
            def _():
                for s in range(1, nx):
                    remote(e2.at[p ^ s], e2.at[p ^ s], s_e.at[s], r_e.at[s], gx=p ^ s).wait_recv()
                total = e2[0]
                for s in range(1, nx):
                    total = total + e2[s]
                e3[place] = total
                for copy in e_line:
                    copy.start()

            @pl.when(d < ny)
            def _():
                third(q, d)

            @pl.when(jnp.logical_and(start, d >= 2))
            def _():
                merge(q, d - 2)

        loop(ny + 2, step)

    def stage(t, lag, act):
        @pl.when(jnp.logical_and(t >= lag, t < chunks + lag))
        def _():
            act(t - lag)

    def tail(t):
        stage(t, 0, lambda q: when(works, lambda: leave(q)))
        stage(t, 1, spread)

        @pl.when(jnp.logical_and(works, jnp.logical_and(t >= 1, t < chunks)))
        def _():
            loop(ny, lambda d: merge(t, d))

        stage(t, 2, fourth)
        stage(t, 3, finish)

    loop(chunks + 3, tail)

    for side in range(2):
        @pl.when(mid - 1 + side != z)
        def _(side=side):
            remote(e3.at[side], e3.at[side], s_e.at[0], r_e.at[nx + side], gy=(z + 1) % ny).wait_recv()

    total = e3[0] + e3[1]
    energy[0] = jnp.sum(total)

    swap_bx.wait_send()
    for copy in eigs:
        copy.wait_send()

    @pl.when(works)
    def _():
        for copy in [e_core] + e_plane + e_line:
            copy.wait_send()

    def plane_drain(zs):
        sent = byb.at[zs, pl.ds(0, 2 * nb - 1)]
        remote(sent, sent, s_byp.at[row_of(zs)], r_byp.at[0, 0, 0], gx=p ^ 1).wait_send()

    def drain(zs):
        for up in (True, False):
            from_here = zs <= z if up else zs >= z

            @pl.when(jnp.logical_and(goes_on(up), from_here))
            def _(up=up):
                bx_line(zs, up).wait_send()

        bx_pass(zs).wait_send()
        for part in range(2):
            for copy in g_copies(zs, part):
                copy.wait_send()
        same = (zs < mid) == low
        when(jnp.logical_or(zs == z, jnp.logical_and(works, jnp.logical_not(same))), lambda: plane_drain(zs))
        when(jnp.logical_and(works, same), lambda: by_cross(zs).wait_send())

        @pl.when(jnp.logical_and(jnp.logical_and(jnp.logical_not(works), same), jnp.where(low, zs <= z, zs >= z)))
        def _():
            for t in range(nx):
                for part in range(2):
                    by_full(zs, t, part).wait_send()

        when(home(zs) != z, lambda: g_send(zs).wait_send())

    loop(ny, drain)

    def drain_chunk(q):
        @pl.when(works)
        def _():
            lanes = cols(q * yq, yq)
            passed_on, sent = vrecv.at[:, :, :, :, lanes], vrecv.at[pl.ds(0, ny - 1), :, :, :, lanes]
            remote(passed_on, passed_on, s_vd.at[q], r_vd.at[q, 0], gz=other).wait_send()
            remote(sent, sent, s_va.at[q], r_va.at[q, 0], gy=(z + 1) % ny).wait_send()

        for side in range(2):
            for copy in v_copies(q, side):
                copy.wait_send()

        def tile(m):
            s_copy(q, m).wait_send()
            out_copy(q, m).wait()

        loop(xb // mt, tile)

    loop(chunks, drain_chunk)


def shards(nx, ny, rhs, basis_x, basis_y, eig_x, eig_y, eig_z):
    xb, yb = rhs.shape[1], rhs.shape[2]
    cx, cy = basis_x.shape[1], basis_y.shape[1]
    nb, ci = nx // 2, cx // 2
    ib = ci // nb
    yq = min(yb, 256)
    chunks, mid, tiles = yb // yq, ny // 2, xb // min(xb, 512)
    ex = eig_x.reshape(xb // LANES, LANES)
    ey = eig_y.reshape(yb // LANES, LANES)
    ez = eig_z.reshape(1, 1)
    dma = pltpu.SemaphoreType.DMA
    any_space, vmem = pl.BlockSpec(memory_space=pl.ANY), pl.BlockSpec(memory_space=pltpu.VMEM)
    solution, energy = pl.pallas_call(
        functools.partial(kernel, nx, ny, yq),
        name="solve",
        out_shape=(
            jax.ShapeDtypeStruct(rhs.shape, BF16),
            jax.ShapeDtypeStruct((1,), F32),
        ),
        in_specs=[any_space] * 3 + [vmem] * 3,
        out_specs=(any_space, pl.BlockSpec(memory_space=pltpu.SMEM)),
        scratch_shapes=[
            pltpu.VMEM((ny, 2, 2 * xb, ci), BF16),
            pltpu.VMEM((ny, nx, yb, cy), BF16),
            pltpu.VMEM((2 * xb, yb), BF16),
            pltpu.VMEM((ny, nb, 2, ib, yb), BF16),
            pltpu.VMEM((ny, nb - 1, 2, ib, yb), BF16),
            pltpu.VMEM((ny, 2, mid, 2, ib, yb), BF16),
            pltpu.VMEM((nx, 2, 2 * mid * ib, cy), BF16),
            pltpu.VMEM((ny, mid, 2, ib, yb), BF16),
            pltpu.VMEM((chunks, ny, 2, nb * ib, yq), BF16),
            pltpu.VMEM((xb, yb), F32),
            pltpu.VMEM((xb, yb), BF16),
            pltpu.VMEM((nx, xb // LANES, LANES), F32),
            pltpu.VMEM((ny, yb // LANES, LANES), F32),
            pltpu.VMEM((2, 8, LANES), F32),
            pltpu.VMEM((2, 2 * mid * ib, LANES), F32),
            pltpu.VMEM((8, LANES), F32),
            pltpu.VMEM((8, LANES), F32),
            pltpu.VMEM((nx, 8, LANES), F32),
            pltpu.VMEM((2, 8, LANES), F32),
            dma((5,)),
            dma((nx + ny,)), dma((nx + ny,)),
            dma((3,)), dma((3,)),
            dma((ny, 2)), dma((ny,)),
            dma((ny,)), dma((ny,)),
            dma((mid, nx, 2)), dma((mid, nx, 2)),
            dma((mid,)), dma((mid,)),
            dma((mid + 1,)), dma((mid + 1, nx - 1, 2)),
            dma((ny, 2, nb - 1)), dma((ny, 2, nb - 1)),
            dma((ny,)), dma((ny, mid)),
            pltpu.SemaphoreType.DMA, dma((ny, mid)),
            dma((chunks,)), dma((chunks, ny)),
            dma((chunks,)), dma((chunks, 2)),
            dma((chunks, 2, nb - 1)), dma((chunks, 2, nb - 1)),
            dma((chunks, tiles)), dma((chunks, tiles)),
            dma((chunks, tiles)),
            dma((nx + ny,)), dma((nx + ny,)),
        ],
        compiler_params=pltpu.CompilerParams(
            collective_id=0, has_side_effects=True, vmem_limit_bytes=65472 * 1024
        ),
    )(rhs, basis_x, basis_y, ex, ey, ez)
    return solution, energy.reshape(())


def solution(mesh):
    return jax.shard_map(
        functools.partial(shards, mesh.shape["gx"], mesh.shape["gy"]),
        mesh=mesh,
        in_specs=(
            P("gz", "gx", "gy"),
            P("gx", ("gy", "gz")),
            P("gy", ("gx", "gz")),
            P("gx"),
            P("gy"),
            P("gz"),
        ),
        out_specs=(P("gz", "gx", "gy"), P()),
        check_vma=False,
    )
```
